16 devices in a mesh: dp: 2 (over y, z), tp: 8 (over x, core).
Axes of the slice: x: 4, y: 2, z: 1, core: 2. Of those that a mesh axis runs over, the one named last changes fastest.
The devices are a block of a 4x4x8 slice.
Arguments:
- token_ids: int32 [4, 256], P('dp'), parts along dimension 0
- emb_table: bfloat16 [2048, 3584], P('tp')
- gain_vec: bfloat16 [3584], replicated
- w_qkv: bfloat16 [3584, 36864], P(None, 'tp')
- grad_u: bfloat16 [4, 256, 36864], P('dp', None, 'tp'), parts along dimension 0
- grad_res: bfloat16 [4, 256, 3584], P('dp', 'tp'), parts along dimension 0
Outputs:
- output 1: bfloat16 [4, 256, 36864], P('dp', None, 'tp'), parts along dimension 0
- output 2: bfloat16 [4, 256, 3584], P('dp', 'tp'), parts along dimension 0
- output 3: float32 [4096, 3584], P(('dp', 'tp')), parts along dimension 0
- output 4: float32 [3584, 73728], P(None, ('dp', 'tp')), parts along dimension 1
- output 5: float32 [7168], P('dp'), parts along dimension 0
There are 2 independent parts. The reference program is written for one: setup_inputs(seed, part) draws one part's arguments, and reference() takes and returns one part's arrays. A program takes and returns all parts, laid end to end along the dimension named above; an argument that names none is the same for every part.
All inputs are finite; a program needn't handle non-finite values.
Results may differ from the reference program's by a relative error of at most 0.001.
Values are sent between devices in bfloat16 or wider.
A program may use at most 768 MiB of HBM per device.

```python
import jax
import jax.numpy as jnp
from jax import lax

NUM_MICRO = 2
SEQ_LEN = 256
VOCAB_ROWS = 2048
MODEL_DIM = 3584
QKV_COLS = 36864
GROUP_SIZE = 8
COLS_DEV = QKV_COLS // GROUP_SIZE
NORM_EPS = 1e-6


def setup_inputs(seed: int = 0, part: int = 0) -> dict:
    root_key = jax.random.key(seed)
    own_keys = jax.random.split(jax.random.fold_in(root_key, part), 6)
    shared_keys = jax.random.split(root_key, 3)
    spacing = VOCAB_ROWS // 64
    base_ids = jax.random.randint(own_keys[0], (NUM_MICRO, SEQ_LEN), 0, VOCAB_ROWS)
    hot_slot = jax.random.randint(own_keys[1], (NUM_MICRO, SEQ_LEN), 0, 64)
    hot_shift = jax.random.randint(own_keys[2], (), 0, spacing)
    use_hot = jax.random.randint(own_keys[3], (NUM_MICRO, SEQ_LEN), 0, 2)
    token_ids = jnp.where(use_hot == 1, hot_slot * spacing + hot_shift, base_ids)
    token_ids = token_ids.at[0, 0].set(0).at[0, 1].set(VOCAB_ROWS - 1).astype(jnp.int32)
    emb_table = jax.random.normal(shared_keys[0], (VOCAB_ROWS, MODEL_DIM), jnp.float32).astype(jnp.bfloat16)
    gain_vec = (0.5 + jax.random.uniform(shared_keys[1], (MODEL_DIM,), jnp.float32)).astype(jnp.bfloat16)
    w_qkv = (jax.random.normal(shared_keys[2], (MODEL_DIM, QKV_COLS), jnp.float32) * MODEL_DIM ** -0.5).astype(jnp.bfloat16)
    grad_u = (jax.random.normal(own_keys[4], (NUM_MICRO, SEQ_LEN, QKV_COLS), jnp.float32) * (MODEL_DIM / QKV_COLS) ** 0.5).astype(jnp.bfloat16)
    grad_res = jax.random.normal(own_keys[5], (NUM_MICRO, SEQ_LEN, MODEL_DIM), jnp.float32).astype(jnp.bfloat16)
    return {'token_ids': token_ids, 'emb_table': emb_table, 'gain_vec': gain_vec, 'w_qkv': w_qkv, 'grad_u': grad_u, 'grad_res': grad_res}


def reference(token_ids, emb_table, gain_vec, w_qkv, grad_u, grad_res):
    gain_f = gain_vec.astype(jnp.float32)

    def micro_step(acc_state, inputs):
        grad_table, grad_w, grad_gain = acc_state
        tok_ids, du_m, dres_m = inputs
        tokens = jnp.take(emb_table, tok_ids, axis=0)
        tok_f = tokens.astype(jnp.float32)
        inv_rms = lax.rsqrt(jnp.mean(tok_f * tok_f, axis=-1, keepdims=True) + NORM_EPS)
        n_hat = tok_f * inv_rms
        normed = (n_hat * gain_f).astype(jnp.bfloat16)
        u_m = jnp.dot(normed, w_qkv, preferred_element_type=jnp.float32).astype(jnp.bfloat16)

        def group_term(dn_acc, group_idx):
            du_r = lax.dynamic_slice_in_dim(du_m, group_idx * COLS_DEV, COLS_DEV, axis=1)
            w_r = lax.dynamic_slice_in_dim(w_qkv, group_idx * COLS_DEV, COLS_DEV, axis=1)
            part_dn = jnp.dot(du_r, w_r.T, preferred_element_type=jnp.float32).astype(jnp.bfloat16)
            return dn_acc + part_dn.astype(jnp.float32), None

        d_norm, _ = lax.scan(group_term, jnp.zeros((SEQ_LEN, MODEL_DIM), jnp.float32), jnp.arange(GROUP_SIZE))
        gain_dn = gain_f * d_norm
        centre = jnp.mean(n_hat * gain_dn, axis=-1, keepdims=True)
        d_x = (dres_m.astype(jnp.float32) + inv_rms * (gain_dn - n_hat * centre)).astype(jnp.bfloat16)
        grad_table = grad_table + jax.ops.segment_sum(d_x.astype(jnp.float32), tok_ids, num_segments=VOCAB_ROWS)
        grad_w = grad_w + jnp.dot(normed.T, du_m, preferred_element_type=jnp.float32)
        grad_gain = grad_gain + jnp.sum(d_norm * n_hat, axis=0)
        return (grad_table, grad_w, grad_gain), (u_m, tokens)

    init_state = (jnp.zeros((VOCAB_ROWS, MODEL_DIM), jnp.float32), jnp.zeros((MODEL_DIM, QKV_COLS), jnp.float32), jnp.zeros((MODEL_DIM,), jnp.float32))
    (grad_table, grad_w, grad_gain), (u_proj, x_resid) = lax.scan(micro_step, init_state, (token_ids, grad_u, grad_res))
    return u_proj, x_resid, grad_table, grad_w, grad_gain
```

```python
import jax
import jax.numpy as jnp
from jax import lax
from jax.sharding import PartitionSpec as P

NORM_EPS = 1e-6


def solution(mesh):
    group_size = mesh.shape['tp']

    def local_step(token_ids, table_loc, gain_vec, w_loc, du_loc, dres_loc):
        micro, seq_len = token_ids.shape
        rows_loc, model_dim = table_loc.shape
        seq_loc = seq_len // group_size
        cols_loc = w_loc.shape[1]
        own = micro * seq_loc
        total = micro * seq_len
        dev_idx = lax.axis_index('tp')
        gain_f = gain_vec.astype(jnp.float32)

        ids = token_ids.reshape(micro, group_size, seq_loc).transpose(1, 0, 2).reshape(total)
        local_ids = ids - dev_idx * rows_loc
        onehot = (lax.broadcasted_iota(jnp.int32, (total, rows_loc), 1) == local_ids[:, None]).astype(jnp.bfloat16)

        partial_x = jnp.dot(onehot, table_loc, preferred_element_type=jnp.float32).astype(jnp.bfloat16)
        x_own = lax.psum_scatter(partial_x, 'tp', scatter_dimension=0, tiled=True)
        x_all = lax.all_gather(x_own, 'tp', axis=0, tiled=True)

        tok_f = x_all.astype(jnp.float32)
        inv_rms = lax.rsqrt(jnp.mean(tok_f * tok_f, axis=-1, keepdims=True) + NORM_EPS)
        normed = (tok_f * inv_rms * gain_f).astype(jnp.bfloat16)
        normed = normed.reshape(group_size, micro, seq_loc, model_dim).transpose(1, 0, 2, 3).reshape(total, model_dim)

        du_flat = du_loc.reshape(total, cols_loc)
        dn_part = lax.dot_general(du_flat, w_loc, (((1,), (1,)), ((), ())), preferred_element_type=jnp.float32).astype(jnp.bfloat16)
        dn_send = dn_part.reshape(micro, group_size, seq_loc, model_dim).transpose(1, 0, 2, 3)
        dn_recv = lax.all_to_all(dn_send, 'tp', 0, 0, tiled=True)
        d_norm = jnp.sum(dn_recv.reshape(group_size, own, model_dim), axis=0, dtype=jnp.float32)

        u = jnp.dot(normed, w_loc, preferred_element_type=jnp.float32).astype(jnp.bfloat16)
        grad_w = lax.dot_general(normed, du_flat, (((0,), (0,)), ((), ())), preferred_element_type=jnp.float32)

        own_f = x_own.astype(jnp.float32)
        inv_own = lax.rsqrt(jnp.mean(own_f * own_f, axis=-1, keepdims=True) + NORM_EPS)
        hat_own = own_f * inv_own
        gain_dn = gain_f * d_norm
        centre = jnp.mean(hat_own * gain_dn, axis=-1, keepdims=True)
        dres_own = dres_loc.reshape(own, model_dim).astype(jnp.float32)
        d_x = (dres_own + inv_own * (gain_dn - hat_own * centre)).astype(jnp.bfloat16)
        grad_gain = lax.psum(jnp.sum(d_norm * hat_own, axis=0), 'tp')
        dx_all = lax.all_gather(d_x, 'tp', axis=0, tiled=True)
        grad_table = lax.dot_general(onehot, dx_all, (((0,), (0,)), ((), ())), preferred_element_type=jnp.float32)
        return (u.reshape(micro, seq_len, cols_loc), x_own.reshape(micro, seq_loc, model_dim),
                grad_table, grad_w, grad_gain)

    return jax.shard_map(local_step, mesh=mesh,
                         in_specs=(P('dp', None), P('tp', None), P(None), P(None, 'tp'), P('dp', None, 'tp'), P('dp', 'tp', None)),
                         out_specs=(P('dp', None, 'tp'), P('dp', 'tp', None), P(('dp', 'tp'), None), P(None, ('dp', 'tp')), P('dp')),
                         check_vma=False)
```

```python
import jax
import jax.numpy as jnp
from jax import lax
from jax.sharding import PartitionSpec as P

NORM_EPS = 1e-6


def solution(mesh):
    group = mesh.shape['tp']
    chips = group // 2
    plus = [(r, (r + 2) % group) for r in range(group)]
    minus = [(r, (r - 2) % group) for r in range(group)]
    opposite = [(r, (r + 4) % group) for r in range(group)]
    swap = [(r, r ^ 1) for r in range(group)]

    def send(value, perm):
        return lax.ppermute(value, 'tp', perm)

    def local_step(token_ids, table_loc, gain_vec, w_loc, du_loc, dres_loc):
        micro, seq_len = token_ids.shape
        rows_loc, model_dim = table_loc.shape
        cols_loc = w_loc.shape[1]
        half = model_dim // 2
        chip_tok = seq_len // chips
        own_tok = chip_tok // 2
        total = micro * seq_len
        dev = lax.axis_index('tp')
        chip, core = dev // 2, dev % 2

        def my_half(value):
            return lax.dynamic_slice_in_dim(value, core * half, half, axis=value.ndim - 1)

        def other_half(value):
            return lax.dynamic_slice_in_dim(value, (1 - core) * half, half, axis=value.ndim - 1)

        def join(mine, other):
            return jnp.where(core == 0, jnp.concatenate([mine, other], -1), jnp.concatenate([other, mine], -1))

        def gather_ring(mine):
            left = send(mine, plus)
            right = send(mine, minus)
            far0 = send(left[0], plus)
            far1 = send(right[1], minus)
            return jnp.stack([mine, right, jnp.stack([far0, far1]), left])

        def reduce_ring(piece):
            relay1 = send(piece(2, 1), plus)
            relay0 = send(piece(2, 0), minus)
            direct0 = send(piece(1, 0), plus)
            direct1 = send(piece(3, 1), minus)
            comb1 = send(piece(1, 1) + relay1, plus)
            comb0 = send(piece(3, 0) + relay0, minus)
            return jnp.stack([piece(0, 0) + direct0 + comb0, piece(0, 1) + direct1 + comb1])

        ids4 = token_ids.reshape(micro, chips, chip_tok)
        ids_rel = jnp.stack([lax.dynamic_index_in_dim(ids4, (chip + j) % chips, 1, keepdims=False) for j in range(chips)]).reshape(total)

        table_partner = send(other_half(table_loc), swap)
        table_chip = jnp.concatenate([my_half(table_loc), table_partner], 0)
        row_iota = lax.broadcasted_iota(jnp.int32, (total, rows_loc), 1)
        hot_own = (row_iota == (ids_rel - dev * rows_loc)[:, None]).astype(jnp.bfloat16)
        hot_partner = (row_iota == (ids_rel - (dev + 1 - 2 * core) * rows_loc)[:, None]).astype(jnp.bfloat16)
        looked = jnp.dot(jnp.concatenate([hot_own, hot_partner], 1), table_chip, preferred_element_type=jnp.float32).astype(jnp.bfloat16)
        looked = looked.reshape(chips, micro, chip_tok, half)

        x_mine = reduce_ring(lambda j, m: looked[j, m])

        du_flat = du_loc.reshape(total, cols_loc)
        dn_part = lax.dot_general(du_flat, w_loc, (((1,), (1,)), ((), ())), preferred_element_type=jnp.float32).astype(jnp.bfloat16)
        dn_partner = send(other_half(dn_part), swap)
        dn4 = my_half(dn_part).reshape(micro, chips, chip_tok, half)
        dp4 = dn_partner.reshape(micro, chips, chip_tok, half)

        x_half = gather_ring(x_mine)
        x_other = send(x_half, swap)
        x_rel = join(x_half, x_other)

        tok_f = x_rel.astype(jnp.float32)
        inv_rms = lax.rsqrt(jnp.mean(tok_f * tok_f, axis=-1, keepdims=True) + NORM_EPS)
        normed = (tok_f * inv_rms * gain_vec.astype(jnp.float32)).astype(jnp.bfloat16)
        normed = lax.dynamic_slice_in_dim(jnp.concatenate([normed, normed], 0), (chips - chip) % chips, chips, axis=0)
        normed = normed.transpose(1, 0, 2, 3).reshape(total, model_dim)

        u = jnp.dot(normed, w_loc, preferred_element_type=jnp.float32).astype(jnp.bfloat16)
        grad_w = lax.dot_general(normed, du_flat, (((0,), (0,)), ((), ())), preferred_element_type=jnp.float32)

        def dn_piece(j, m):
            d = (chip + j) % chips
            return (lax.dynamic_index_in_dim(dn4[m], d, 0, keepdims=False).astype(jnp.float32)
                    + lax.dynamic_index_in_dim(dp4[m], d, 0, keepdims=False).astype(jnp.float32))

        d_norm = reduce_ring(dn_piece)
        gain_half = my_half(gain_vec).astype(jnp.float32)
        hat = x_mine.astype(jnp.float32) * inv_rms[0]
        gain_dn = gain_half * d_norm
        dot_mine = jnp.sum(hat * gain_dn, axis=-1)
        centre = ((dot_mine + send(dot_mine, swap)) / model_dim)[..., None]
        dres_other = send(other_half(dres_loc), swap)
        dres_mine = my_half(dres_loc)
        first = jnp.where(core == 0, dres_mine, dres_other)
        second = jnp.where(core == 0, dres_other, dres_mine)
        dres_chip = jnp.concatenate([first, second], 1).astype(jnp.float32)
        d_x = (dres_chip + inv_rms[0] * (gain_dn - hat * centre)).astype(jnp.bfloat16)

        gg = jnp.sum(d_norm * hat, axis=(0, 1))
        gg = gg + send(gg, plus)
        gg = gg + send(gg, opposite)
        grad_gain = join(gg, send(gg, swap))

        dx_half = gather_ring(d_x)
        dx_other = send(dx_half, swap)
        dx_rel = join(dx_half, dx_other).reshape(total, model_dim)
        grad_table = lax.dot_general(hot_own, dx_rel, (((0,), (0,)), ((), ())), preferred_element_type=jnp.float32)
        x_own = lax.dynamic_slice_in_dim(x_rel[0], core * own_tok, own_tok, axis=1)
        return u.reshape(micro, seq_len, cols_loc), x_own, grad_table, grad_w, grad_gain

    return jax.shard_map(local_step, mesh=mesh,
                         in_specs=(P('dp', None), P('tp', None), P(None), P(None, 'tp'), P('dp', None, 'tp'), P('dp', 'tp', None)),
                         out_specs=(P('dp', None, 'tp'), P('dp', 'tp', None), P(('dp', 'tp'), None), P(None, ('dp', 'tp')), P('dp')),
                         check_vma=False)
```

```python
import functools

import jax
import jax.numpy as jnp
from jax import lax
from jax.experimental import pallas as pl
from jax.experimental.pallas import tpu as pltpu
from jax.sharding import PartitionSpec as P

NORM_EPS = 1e-6
MESH = pl.DeviceIdType.MESH
F32 = jnp.float32
BF16 = jnp.bfloat16
DN_TILE = 256
RELAY_AT = (3, 5)
SUM_AT = (10, 12)


def gather_kernel(group, ids_ref, gain_ref, table_ref, w_ref, du_ref,
                  n_out, xchip_out, s_out,
                  tab, looked, r_relay, r_direct, r_comb, s_comb, xbuf, n_v, du_v, wbuf, dn2, dnp, stage,
                  lsem, wsem, osem, snd, rcv):
    dev = lax.axis_index('tp')
    chips = group // 2
    chip = lax.div(dev, 2)
    core = lax.rem(dev, 2)
    plus = lax.rem(dev + 2, group)
    minus = lax.rem(dev + group - 2, group)
    partner = dev + 1 - 2 * core
    micro, seq_len = ids_ref.shape
    rows_loc, model_dim = table_ref.shape
    half = model_dim // 2
    ctok = seq_len // chips
    qrows = ctok // 2
    tiles = half // DN_TILE
    my_cols = pl.ds(pl.multiple_of(core * half, 128), half)
    his_cols = pl.ds(pl.multiple_of((1 - core) * half, 128), half)

    def rel(j):
        return lax.rem(chip + j, chips)

    def tok(d, q=None):
        if q is None:
            return pl.ds(pl.multiple_of(d * ctok, ctok), ctok)
        return pl.ds(pl.multiple_of(d * ctok + q * qrows, qrows), qrows)

    def remote(src, dst, slot, target):
        return pltpu.make_async_remote_copy(src_ref=src, dst_ref=dst, send_sem=snd.at[slot], recv_sem=rcv.at[slot],
                                            device_id={'tp': target}, device_id_type=MESH)

    cp_du = pltpu.make_async_copy(du_ref, du_v, lsem.at[0])
    cp_tab = pltpu.make_async_copy(table_ref.at[:, my_cols],
                                   tab.at[pl.ds(pl.multiple_of(core * rows_loc, rows_loc), rows_loc)], lsem.at[1])

    def w_copy(t):
        ft = jnp.where(t < tiles, (1 - core) * tiles + t, core * tiles + t - tiles)
        slot = lax.rem(t, 2)
        return pltpu.make_async_copy(w_ref.at[pl.ds(pl.multiple_of(ft * DN_TILE, DN_TILE), DN_TILE), :], wbuf.at[slot],
                                     wsem.at[slot])

    cp_tab.start()
    cp_du.start()
    w_copy(0).start()

    barrier = pltpu.get_barrier_semaphore()
    for target in (plus, minus, partner):
        pl.semaphore_signal(barrier, inc=1, device_id={'tp': target}, device_id_type=MESH)
    pl.semaphore_wait(barrier, 3)

    table_msg = remote(table_ref.at[:, his_cols], tab.at[pl.ds(pl.multiple_of(core * rows_loc, rows_loc), rows_loc)], 0, partner)
    table_msg.start()

    def relay(m, q):
        return remote(looked.at[m, tok(rel(2), q)], r_relay.at[m, q], 1 + 2 * m + q, minus if m == 0 else plus)

    def direct(m, q):
        return remote(looked.at[m, tok(rel(1 if m == 0 else 3), q)], r_direct.at[m, q], 5 + 2 * m + q, plus if m == 0 else minus)

    def comb(m, q):
        return remote(s_comb.at[m, q], r_comb.at[m, q], 9 + 2 * m + q, minus if m == 0 else plus)

    def spread(q, way):
        here = xbuf.at[:, tok(chip, q), my_cols]
        return remote(here, here, 13 + 3 * q + way, (plus, minus, partner)[way])

    def far(q, m):
        here = xbuf.at[m, tok(rel(3 if m == 0 else 1), q), my_cols]
        return remote(here, here, 19 + 2 * q + m, plus if m == 0 else minus)

    def near_fwd(q, side):
        here = xbuf.at[:, tok(rel(3 if side == 0 else 1), q), my_cols]
        return remote(here, here, 23 + 2 * q + side, partner)

    def far_fwd(q, m):
        here = xbuf.at[m, tok(rel(2), q), my_cols]
        return remote(here, here, 27 + 2 * q + m, partner)

    def dn_msg(t):
        cols = pl.ds(pl.multiple_of(t * DN_TILE, DN_TILE), DN_TILE)
        return remote(dn2.at[0, :, :, cols], dnp.at[:, :, cols], 31 + t, partner)

    cp_tab.wait()
    table_msg.wait_recv()
    row_id = lax.broadcasted_iota(jnp.int32, (2 * rows_loc, seq_len), 0) + chip * (2 * rows_loc)
    for m in (1, 0):
        hot = jnp.where(row_id == ids_ref[m:m + 1, :], 1.0, 0.0).astype(BF16)
        looked[m] = lax.dot_general(hot, tab[...], (((0,), (0,)), ((), ())), preferred_element_type=F32).astype(BF16)
    for q in range(2):
        for m in range(2):
            relay(m, q).start()
    for q in range(2):
        for m in range(2):
            direct(m, q).start()
    cp_du.wait()

    def relay_step(q):
        for m in range(2):
            relay(m, q).wait_recv()
            s_comb[m, q] = looked[m, tok(rel(3 if m == 0 else 1), q)] + r_relay[m, q]
            comb(m, q).start()

    def sum_step(q):
        for m in range(2):
            direct(m, q).wait_recv()
            comb(m, q).wait_recv()
            xbuf[m, tok(chip, q), my_cols] = (looked[m, tok(chip, q)] + r_direct[m, q]) + r_comb[m, q]
        for way in range(3):
            spread(q, way).start()

    def dn_step(t, carry):
        @pl.when(t + 1 < 2 * tiles)
        def _():
            w_copy(t + 1).start()
        w_copy(t).wait()
        slot = lax.rem(t, 2)
        part = lax.dot_general(du_v[...].reshape(micro * seq_len, du_v.shape[2]), wbuf[slot], (((1,), (1,)), ((), ())),
                               preferred_element_type=F32).astype(BF16).reshape(micro, seq_len, DN_TILE)
        side = lax.div(t, tiles)
        col = (t - side * tiles) * DN_TILE
        dn2[side, :, :, pl.ds(pl.multiple_of(col, DN_TILE), DN_TILE)] = part

        @pl.when(t < tiles)
        def _():
            dn_msg(t).start()
        for q in range(2):
            @pl.when(t == RELAY_AT[q])
            def _():
                relay_step(q)
        for q in range(2):
            @pl.when(t == SUM_AT[q])
            def _():
                sum_step(q)
        return carry

    lax.fori_loop(0, 2 * tiles, dn_step, 0)

    def dn_wait(t, carry):
        dn_msg(t).wait_recv()
        return carry
    lax.fori_loop(0, tiles, dn_wait, 0)

    def s_copy(i):
        return pltpu.make_async_copy(stage.at[i], s_out.at[i], osem.at[i])

    def s_step(i, carry):
        j, m = lax.div(i, 2), lax.rem(i, 2)
        rows = tok(rel(j))
        stage[i] = dn2[1, m, rows].astype(F32) + dnp[m, rows].astype(F32)
        s_copy(i).start()
        return carry

    def near_step(q):
        spread(q, 0).wait_recv()
        far(q, 0).start()
        near_fwd(q, 0).start()
        spread(q, 1).wait_recv()
        far(q, 1).start()
        near_fwd(q, 1).start()

    near_step(0)
    lax.fori_loop(0, 2 * chips, s_step, 0)
    near_step(1)

    def n_copy(d, i):
        return pltpu.make_async_copy(n_v.at[:, tok(d)], n_out.at[:, tok(d)], osem.at[2 * chips + i])

    def norm_piece(j):
        d = rel(j)

        def body(i, carry):
            m, r = lax.div(i, ctok // 16), lax.rem(i, ctok // 16)
            rows = pl.ds(pl.multiple_of(d * ctok + r * 16, 16), 16)
            xf = xbuf[m, rows].astype(F32)
            inv = lax.rsqrt(jnp.mean(xf * xf, axis=-1, keepdims=True) + NORM_EPS)
            n_v[m, rows] = (xf * inv * gain_ref[...].astype(F32)).astype(BF16)
            return carry
        lax.fori_loop(0, micro * (ctok // 16), body, 0)
        n_copy(d, j).start()

    for q in range(2):
        spread(q, 2).wait_recv()
    cp_x = pltpu.make_async_copy(xbuf.at[:, tok(chip)], xchip_out, lsem.at[0])
    cp_x.start()
    norm_piece(0)
    for q in range(2):
        for m in range(2):
            far(q, m).wait_recv()
            far_fwd(q, m).start()
    for side, j in ((0, 3), (1, 1)):
        for q in range(2):
            near_fwd(q, side).wait_recv()
        norm_piece(j)
    for q in range(2):
        for m in range(2):
            far_fwd(q, m).wait_recv()
    norm_piece(2)

    for i in range(2 * chips):
        s_copy(i).wait()
    for j in range(chips):
        n_copy(rel(j), j).wait()
    cp_x.wait()
    table_msg.wait_send()
    for q in range(2):
        for m in range(2):
            relay(m, q).wait_send()
            direct(m, q).wait_send()
            comb(m, q).wait_send()
            far(q, m).wait_send()
            far_fwd(q, m).wait_send()
            near_fwd(q, m).wait_send()
        for way in range(3):
            spread(q, way).wait_send()

    def dn_drain(t, carry):
        dn_msg(t).wait_send()
        return carry
    lax.fori_loop(0, tiles, dn_drain, 0)


def gather_call(group, ids, gain2, table, w, du):
    micro, seq_len = ids.shape
    rows_loc, model_dim = table.shape
    cols_loc = w.shape[1]
    half = model_dim // 2
    chips = group // 2
    ctok = seq_len // chips
    tiles = half // DN_TILE
    any_spec = pl.BlockSpec(memory_space=pl.ANY)
    vmem_spec = pl.BlockSpec(memory_space=pltpu.VMEM)
    msg = pltpu.VMEM((2, 2, ctok // 2, half), BF16)
    total = micro * seq_len
    return pl.pallas_call(
        functools.partial(gather_kernel, group),
        out_shape=(jax.ShapeDtypeStruct((micro, seq_len, model_dim), BF16),
                   jax.ShapeDtypeStruct((micro, ctok, model_dim), BF16),
                   jax.ShapeDtypeStruct((2 * chips, ctok, half), F32)),
        in_specs=[vmem_spec, vmem_spec, any_spec, any_spec, any_spec],
        out_specs=(any_spec,) * 3,
        scratch_shapes=[
            pltpu.VMEM((2 * rows_loc, half), BF16),
            pltpu.VMEM((micro, seq_len, half), BF16),
            msg, msg, msg, msg,
            pltpu.VMEM((micro, seq_len, model_dim), BF16),
            pltpu.VMEM((micro, seq_len, model_dim), BF16),
            pltpu.VMEM((micro, seq_len, cols_loc), BF16),
            pltpu.VMEM((2, DN_TILE, cols_loc), BF16),
            pltpu.VMEM((2, micro, seq_len, half), BF16),
            pltpu.VMEM((micro, seq_len, half), BF16),
            pltpu.VMEM((2 * chips, ctok, half), F32),
            pltpu.SemaphoreType.DMA((2,)),
            pltpu.SemaphoreType.DMA((2,)),
            pltpu.SemaphoreType.DMA((3 * chips,)),
            pltpu.SemaphoreType.DMA((31 + tiles,)),
            pltpu.SemaphoreType.DMA((31 + tiles,)),
        ],
        compiler_params=pltpu.CompilerParams(collective_id=0, has_side_effects=True, vmem_limit_bytes=58 * 1024 * 1024),
        cost_estimate=pl.CostEstimate(flops=2 * total * cols_loc * model_dim, bytes_accessed=2 * cols_loc * model_dim, transcendentals=0),
        name="gather_dn",
    )(ids, gain2, table, w, du)


def solution(mesh):
    group = mesh.shape['tp']
    chips = group // 2
    plus = [(r, (r + 2) % group) for r in range(group)]
    minus = [(r, (r - 2) % group) for r in range(group)]
    opposite = [(r, (r + 4) % group) for r in range(group)]
    swap = [(r, r ^ 1) for r in range(group)]

    def send(value, perm):
        return lax.ppermute(value, 'tp', perm)

    def local_step(token_ids, table_loc, gain_vec, w_loc, du_loc, dres_loc):
        micro, seq_len = token_ids.shape
        rows_loc, model_dim = table_loc.shape
        cols_loc = w_loc.shape[1]
        half = model_dim // 2
        chip_tok = seq_len // chips
        own_tok = chip_tok // 2
        total = micro * seq_len
        dev = lax.axis_index('tp')
        chip, core = lax.div(dev, 2), lax.rem(dev, 2)

        def my_half(value):
            return lax.dynamic_slice_in_dim(value, core * half, half, axis=value.ndim - 1)

        def other_half(value):
            return lax.dynamic_slice_in_dim(value, (1 - core) * half, half, axis=value.ndim - 1)

        def join(mine, other):
            return jnp.where(core == 0, jnp.concatenate([mine, other], -1), jnp.concatenate([other, mine], -1))

        def gather_ring(mine):
            left = send(mine, plus)
            right = send(mine, minus)
            far0 = send(left[0], plus)
            far1 = send(right[1], minus)
            return jnp.stack([mine, right, jnp.stack([far0, far1]), left])

        normed, x_chip, s_rel = gather_call(group, token_ids, gain_vec.reshape(1, model_dim), table_loc, w_loc, du_loc)

        def reduce_ring(piece):
            relay1 = send(piece(2, 1), plus)
            relay0 = send(piece(2, 0), minus)
            direct0 = send(piece(1, 0), plus)
            direct1 = send(piece(3, 1), minus)
            comb1 = send(piece(1, 1) + relay1, plus)
            comb0 = send(piece(3, 0) + relay0, minus)
            return jnp.stack([piece(0, 0) + direct0 + comb0, piece(0, 1) + direct1 + comb1])

        d_norm = reduce_ring(lambda j, m: s_rel[2 * j + m])
        normed = normed.reshape(total, model_dim)
        du_flat = du_loc.reshape(total, cols_loc)
        u = jnp.dot(normed, w_loc, preferred_element_type=jnp.float32).astype(jnp.bfloat16)
        grad_w = lax.dot_general(normed, du_flat, (((0,), (0,)), ((), ())), preferred_element_type=jnp.float32)

        ids4 = token_ids.reshape(micro, chips, chip_tok)
        ids_rel = jnp.stack([lax.dynamic_index_in_dim(ids4, lax.rem(chip + j, chips), 1, keepdims=False) for j in range(chips)]).reshape(total)
        row_iota = lax.broadcasted_iota(jnp.int32, (total, rows_loc), 1)
        hot_own = (row_iota == (ids_rel - dev * rows_loc)[:, None]).astype(jnp.bfloat16)

        xf = x_chip.astype(jnp.float32)
        inv_rms = lax.rsqrt(jnp.mean(xf * xf, axis=-1, keepdims=True) + NORM_EPS)
        gain_half = my_half(gain_vec).astype(jnp.float32)
        hat = my_half(x_chip).astype(jnp.float32) * inv_rms
        gain_dn = gain_half * d_norm
        dot_mine = jnp.sum(hat * gain_dn, axis=-1)
        centre = ((dot_mine + send(dot_mine, swap)) / model_dim)[..., None]
        dres_other = send(other_half(dres_loc), swap)
        dres_mine = my_half(dres_loc)
        first = jnp.where(core == 0, dres_mine, dres_other)
        second = jnp.where(core == 0, dres_other, dres_mine)
        dres_chip = jnp.concatenate([first, second], 1).astype(jnp.float32)
        d_x = (dres_chip + inv_rms * (gain_dn - hat * centre)).astype(jnp.bfloat16)

        gg = jnp.sum(d_norm * hat, axis=(0, 1))
        gg = gg + send(gg, plus)
        gg = gg + send(gg, opposite)
        grad_gain = join(gg, send(gg, swap))

        dx_half = gather_ring(d_x)
        dx_other = send(dx_half, swap)
        dx_rel = join(dx_half, dx_other).reshape(total, model_dim)
        grad_table = lax.dot_general(hot_own, dx_rel, (((0,), (0,)), ((), ())), preferred_element_type=jnp.float32)
        x_own = lax.dynamic_slice_in_dim(x_chip, core * own_tok, own_tok, axis=1)
        return u.reshape(micro, seq_len, cols_loc), x_own, grad_table, grad_w, grad_gain

    return jax.shard_map(local_step, mesh=mesh,
                         in_specs=(P('dp', None), P('tp', None), P(None), P(None, 'tp'), P('dp', None, 'tp'), P('dp', 'tp', None)),
                         out_specs=(P('dp', None, 'tp'), P('dp', 'tp', None), P(('dp', 'tp'), None), P(None, ('dp', 'tp')), P('dp')),
                         check_vma=False)
```

```python
import functools

import jax
import jax.numpy as jnp
from jax import lax
from jax.experimental import pallas as pl
from jax.experimental.pallas import tpu as pltpu
from jax.sharding import PartitionSpec as P

NORM_EPS = 1e-6
MESH = pl.DeviceIdType.MESH
F32 = jnp.float32
BF16 = jnp.bfloat16
DN_TILE = 256
RELAY_AT = (3, 5)
SUM_AT = (10, 12)
DW_ROWS = 256
U_COLS = 512
U_HOOKS = (2, 3, 4, 5, 6, 7)
DE_COLS = 512


def gather_kernel(group, ids_ref, gain_ref, table_ref, w_ref, du_ref,
                  n_out, xchip_out, plus_out, minus_out, keep_out,
                  tab, looked, r_relay, r_direct, r_comb, s_comb, xbuf, n_v, du_v, wbuf, dn2, dnp, stage,
                  lsem, wsem, osem, snd, rcv):
    dev = lax.axis_index('tp')
    chips = group // 2
    chip = lax.div(dev, 2)
    core = lax.rem(dev, 2)
    plus = lax.rem(dev + 2, group)
    minus = lax.rem(dev + group - 2, group)
    partner = dev + 1 - 2 * core
    micro, seq_len = ids_ref.shape
    rows_loc, model_dim = table_ref.shape
    half = model_dim // 2
    ctok = seq_len // chips
    qrows = ctok // 2
    tiles = half // DN_TILE
    my_cols = pl.ds(pl.multiple_of(core * half, 128), half)
    his_cols = pl.ds(pl.multiple_of((1 - core) * half, 128), half)

    def rel(j):
        return lax.rem(chip + j, chips)

    def tok(d, q=None):
        if q is None:
            return pl.ds(pl.multiple_of(d * ctok, ctok), ctok)
        return pl.ds(pl.multiple_of(d * ctok + q * qrows, qrows), qrows)

    def remote(src, dst, slot, target):
        return pltpu.make_async_remote_copy(src_ref=src, dst_ref=dst, send_sem=snd.at[slot], recv_sem=rcv.at[slot],
                                            device_id={'tp': target}, device_id_type=MESH)

    cp_du = pltpu.make_async_copy(du_ref, du_v, lsem.at[0])
    cp_tab = pltpu.make_async_copy(table_ref.at[:, my_cols],
                                   tab.at[pl.ds(pl.multiple_of(core * rows_loc, rows_loc), rows_loc)], lsem.at[1])

    def w_copy(t):
        ft = jnp.where(t < tiles, (1 - core) * tiles + t, core * tiles + t - tiles)
        slot = lax.rem(t, 2)
        return pltpu.make_async_copy(w_ref.at[pl.ds(pl.multiple_of(ft * DN_TILE, DN_TILE), DN_TILE), :], wbuf.at[slot],
                                     wsem.at[slot])

    cp_tab.start()
    cp_du.start()
    w_copy(0).start()

    barrier = pltpu.get_barrier_semaphore()
    for target in (plus, minus, partner):
        pl.semaphore_signal(barrier, inc=1, device_id={'tp': target}, device_id_type=MESH)
    pl.semaphore_wait(barrier, 3)

    table_msg = remote(table_ref.at[:, his_cols], tab.at[pl.ds(pl.multiple_of(core * rows_loc, rows_loc), rows_loc)], 0, partner)
    table_msg.start()

    def relay(m, q):
        return remote(looked.at[m, tok(rel(2), q)], r_relay.at[m, q], 1 + 2 * m + q, minus if m == 0 else plus)

    def direct(m, q):
        return remote(looked.at[m, tok(rel(1 if m == 0 else 3), q)], r_direct.at[m, q], 5 + 2 * m + q, plus if m == 0 else minus)

    def comb(m, q):
        return remote(s_comb.at[m, q], r_comb.at[m, q], 9 + 2 * m + q, minus if m == 0 else plus)

    def spread(q, way):
        here = xbuf.at[:, tok(chip, q), my_cols]
        return remote(here, here, 13 + 3 * q + way, (plus, minus, partner)[way])

    def far(q, m):
        here = xbuf.at[m, tok(rel(3 if m == 0 else 1), q), my_cols]
        return remote(here, here, 19 + 2 * q + m, plus if m == 0 else minus)

    def near_fwd(q, side):
        here = xbuf.at[:, tok(rel(3 if side == 0 else 1), q), my_cols]
        return remote(here, here, 23 + 2 * q + side, partner)

    def far_fwd(q, m):
        here = xbuf.at[m, tok(rel(2), q), my_cols]
        return remote(here, here, 27 + 2 * q + m, partner)

    def dn_msg(t):
        cols = pl.ds(pl.multiple_of(t * DN_TILE, DN_TILE), DN_TILE)
        return remote(dn2.at[0, :, :, cols], dnp.at[:, :, cols], 31 + t, partner)

    cp_tab.wait()
    table_msg.wait_recv()
    row_id = lax.broadcasted_iota(jnp.int32, (2 * rows_loc, seq_len), 0) + chip * (2 * rows_loc)
    for m in (1, 0):
        hot = jnp.where(row_id == ids_ref[m:m + 1, :], 1.0, 0.0).astype(BF16)
        looked[m] = lax.dot_general(hot, tab[...], (((0,), (0,)), ((), ())), preferred_element_type=F32).astype(BF16)
    for q in range(2):
        for m in range(2):
            relay(m, q).start()
    for q in range(2):
        for m in range(2):
            direct(m, q).start()
    cp_du.wait()

    def relay_step(q):
        for m in range(2):
            relay(m, q).wait_recv()
            s_comb[m, q] = looked[m, tok(rel(3 if m == 0 else 1), q)] + r_relay[m, q]
            comb(m, q).start()

    def sum_step(q):
        for m in range(2):
            direct(m, q).wait_recv()
            comb(m, q).wait_recv()
            xbuf[m, tok(chip, q), my_cols] = (looked[m, tok(chip, q)] + r_direct[m, q]) + r_comb[m, q]
        for way in range(3):
            spread(q, way).start()

    def dn_step(t, carry):
        @pl.when(t + 1 < 2 * tiles)
        def _():
            w_copy(t + 1).start()

        w_copy(t).wait()
        slot = lax.rem(t, 2)
        part = lax.dot_general(du_v[...].reshape(micro * seq_len, du_v.shape[2]), wbuf[slot], (((1,), (1,)), ((), ())),
                               preferred_element_type=F32).astype(BF16).reshape(micro, seq_len, DN_TILE)
        side = lax.div(t, tiles)
        col = (t - side * tiles) * DN_TILE
        dn2[side, :, :, pl.ds(pl.multiple_of(col, DN_TILE), DN_TILE)] = part

        @pl.when(t < tiles)
        def _():
            dn_msg(t).start()

        for q in range(2):
            @pl.when(t == RELAY_AT[q])
            def _():
                relay_step(q)
        for q in range(2):
            @pl.when(t == SUM_AT[q])
            def _():
                sum_step(q)
        return carry

    lax.fori_loop(0, 2 * tiles, dn_step, 0)

    def dn_wait(t, carry):
        dn_msg(t).wait_recv()
        return carry

    lax.fori_loop(0, tiles, dn_wait, 0)

    terms = ((2, 1), (1, 0), (2, 0), (3, 1), (1, 1), (3, 0), (0, 0), (0, 1))

    def s_copy(i):
        out = (plus_out, minus_out, keep_out, keep_out)[i // 2]
        return pltpu.make_async_copy(stage.at[i], out.at[i % 2 if i < 4 else i - 4], osem.at[i])

    def s_steps():
        for i, (j, m) in enumerate(terms):
            stage[i] = dn2[1, m, tok(rel(j))].astype(F32) + dnp[m, tok(rel(j))].astype(F32)
            s_copy(i).start()

    def near_step(q):
        spread(q, 0).wait_recv()
        far(q, 0).start()
        near_fwd(q, 0).start()
        spread(q, 1).wait_recv()
        far(q, 1).start()
        near_fwd(q, 1).start()

    near_step(0)
    s_steps()
    near_step(1)

    def n_copy(d, i):
        return pltpu.make_async_copy(n_v.at[:, tok(d)], n_out.at[:, tok(d)], osem.at[2 * chips + i])

    def norm_piece(j):
        d = rel(j)

        def body(i, carry):
            m, r = lax.div(i, ctok // 16), lax.rem(i, ctok // 16)
            rows = pl.ds(pl.multiple_of(d * ctok + r * 16, 16), 16)
            xf = xbuf[m, rows].astype(F32)
            inv = lax.rsqrt(jnp.mean(xf * xf, axis=-1, keepdims=True) + NORM_EPS)
            n_v[m, rows] = (xf * inv * gain_ref[...].astype(F32)).astype(BF16)
            return carry

        lax.fori_loop(0, micro * (ctok // 16), body, 0)
        n_copy(d, j).start()

    for q in range(2):
        spread(q, 2).wait_recv()
    cp_x = pltpu.make_async_copy(xbuf.at[:, tok(chip)], xchip_out, lsem.at[0])
    cp_x.start()
    norm_piece(0)
    for q in range(2):
        for m in range(2):
            far(q, m).wait_recv()
            far_fwd(q, m).start()
    for side, j in ((0, 3), (1, 1)):
        for q in range(2):
            near_fwd(q, side).wait_recv()
        norm_piece(j)
    for q in range(2):
        for m in range(2):
            far_fwd(q, m).wait_recv()
    norm_piece(2)

    for i in range(2 * chips):
        s_copy(i).wait()
    for j in range(chips):
        n_copy(rel(j), j).wait()
    cp_x.wait()
    table_msg.wait_send()
    for q in range(2):
        for m in range(2):
            relay(m, q).wait_send()
            direct(m, q).wait_send()
            comb(m, q).wait_send()
            far(q, m).wait_send()
            far_fwd(q, m).wait_send()
            near_fwd(q, m).wait_send()
        for way in range(3):
            spread(q, way).wait_send()

    def dn_drain(t, carry):
        dn_msg(t).wait_send()
        return carry

    lax.fori_loop(0, tiles, dn_drain, 0)


def gather_call(group, ids, gain2, table, w, du):
    micro, seq_len = ids.shape
    rows_loc, model_dim = table.shape
    cols_loc = w.shape[1]
    half = model_dim // 2
    chips = group // 2
    ctok = seq_len // chips
    tiles = half // DN_TILE
    any_spec = pl.BlockSpec(memory_space=pl.ANY)
    vmem_spec = pl.BlockSpec(memory_space=pltpu.VMEM)
    msg = pltpu.VMEM((2, 2, ctok // 2, half), BF16)
    total = micro * seq_len
    return pl.pallas_call(
        functools.partial(gather_kernel, group),
        out_shape=(jax.ShapeDtypeStruct((micro, seq_len, model_dim), BF16),
                   jax.ShapeDtypeStruct((micro, ctok, model_dim), BF16),
                   jax.ShapeDtypeStruct((2, ctok, half), F32),
                   jax.ShapeDtypeStruct((2, ctok, half), F32),
                   jax.ShapeDtypeStruct((4, ctok, half), F32)),
        in_specs=[vmem_spec, vmem_spec, any_spec, any_spec, any_spec],
        out_specs=(any_spec,) * 5,
        scratch_shapes=[
            pltpu.VMEM((2 * rows_loc, half), BF16),
            pltpu.VMEM((micro, seq_len, half), BF16),
            msg, msg, msg, msg,
            pltpu.VMEM((micro, seq_len, model_dim), BF16),
            pltpu.VMEM((micro, seq_len, model_dim), BF16),
            pltpu.VMEM((micro, seq_len, cols_loc), BF16),
            pltpu.VMEM((2, DN_TILE, cols_loc), BF16),
            pltpu.VMEM((2, micro, seq_len, half), BF16),
            pltpu.VMEM((micro, seq_len, half), BF16),
            pltpu.VMEM((2 * chips, ctok, half), F32),
            pltpu.SemaphoreType.DMA((2,)),
            pltpu.SemaphoreType.DMA((2,)),
            pltpu.SemaphoreType.DMA((3 * chips,)),
            pltpu.SemaphoreType.DMA((31 + tiles,)),
            pltpu.SemaphoreType.DMA((31 + tiles,)),
        ],
        compiler_params=pltpu.CompilerParams(collective_id=0, has_side_effects=True, vmem_limit_bytes=58 * 1024 * 1024),
        cost_estimate=pl.CostEstimate(flops=2 * total * cols_loc * model_dim, bytes_accessed=2 * cols_loc * model_dim, transcendentals=0),
        name="gather_dn",
    )(ids, gain2, table, w, du)


def weight_grad_kernel(n_ref, du_ref, out_ref):
    out_ref[...] = lax.dot_general(n_ref[...], du_ref[...], (((0,), (0,)), ((), ())), preferred_element_type=F32)


def weight_grad_call(n2, du2):
    total, model_dim = n2.shape
    cols = du2.shape[1]
    return pl.pallas_call(
        weight_grad_kernel,
        grid=(model_dim // DW_ROWS,),
        out_shape=jax.ShapeDtypeStruct((model_dim, cols), F32),
        in_specs=[pl.BlockSpec((total, DW_ROWS), lambda i: (0, i)), pl.BlockSpec((total, cols), lambda i: (0, 0))],
        out_specs=pl.BlockSpec((DW_ROWS, cols), lambda i: (i, 0)),
        compiler_params=pltpu.CompilerParams(dimension_semantics=("arbitrary",), vmem_limit_bytes=40 * 1024 * 1024),
        cost_estimate=pl.CostEstimate(flops=2 * total * cols * model_dim, bytes_accessed=4 * cols * model_dim, transcendentals=0),
        name="weight_grad",
    )(n2, du2)


def finish_kernel(group, ids_ref, gain_ref, rp_ref, rm_ref, keep_ref, xchip_ref, dres_ref, n_ref, w_ref,
                  u_out, de_out, dg_out,
                  rp, rm, keep, xc, dres, n_v, wbuf, ubuf, s_comb, r_comb, dn_v, dot_s, dot_r, dxbuf, dg_v, dg_r, dg_half, de_v,
                  lsem, wsem, usem, osem, snd, rcv):
    dev = lax.axis_index('tp')
    chips = group // 2
    chip = lax.div(dev, 2)
    core = lax.rem(dev, 2)
    plus = lax.rem(dev + 2, group)
    minus = lax.rem(dev + group - 2, group)
    opposite = lax.rem(dev + group // 2, group)
    partner = dev + 1 - 2 * core
    micro, seq_len = ids_ref.shape
    model_dim = gain_ref.shape[1]
    half = model_dim // 2
    ctok = seq_len // chips
    qrows = ctok // 2
    u_cols = wbuf.shape[2]
    steps = w_ref.shape[1] // u_cols
    rows_loc = de_out.shape[0]
    total = micro * seq_len
    my_cols = pl.ds(pl.multiple_of(core * half, 128), half)
    his_cols = pl.ds(pl.multiple_of((1 - core) * half, 128), half)

    def rel(j):
        return lax.rem(chip + j, chips)

    def tok(d, q=None):
        if q is None:
            return pl.ds(pl.multiple_of(d * ctok, ctok), ctok)
        return pl.ds(pl.multiple_of(d * ctok + q * qrows, qrows), qrows)

    def remote(src, dst, slot, target):
        return pltpu.make_async_remote_copy(src_ref=src, dst_ref=dst, send_sem=snd.at[slot], recv_sem=rcv.at[slot],
                                            device_id={'tp': target}, device_id_type=MESH)

    def local(src, dst, i):
        return pltpu.make_async_copy(src, dst, lsem.at[i])

    own_rows = pl.ds(pl.multiple_of(core * qrows, qrows), qrows)
    loads = [local(rp_ref, rp, 0), local(rm_ref, rm, 1), local(keep_ref, keep, 2), local(xchip_ref, xc, 3),
             local(n_ref, n_v, 4), local(dres_ref.at[:, :, my_cols], dres.at[:, own_rows], 5)]
    for cp in loads[:4]:
        cp.start()

    def w_copy(t):
        slot = lax.rem(t, 2)
        return pltpu.make_async_copy(w_ref.at[:, pl.ds(pl.multiple_of(t * u_cols, u_cols), u_cols)], wbuf.at[slot], wsem.at[slot])

    def u_copy(t):
        slot = lax.rem(t, 2)
        return pltpu.make_async_copy(ubuf.at[slot], u_out.at[:, :, pl.ds(pl.multiple_of(t * u_cols, u_cols), u_cols)], usem.at[slot])

    loads[4].start()
    loads[5].start()
    w_copy(0).start()

    barrier = pltpu.get_barrier_semaphore()
    for target in (plus, minus, partner, opposite):
        pl.semaphore_signal(barrier, inc=1, device_id={'tp': target}, device_id_type=MESH)
    pl.semaphore_wait(barrier, 4)

    dres_msg = remote(dres_ref.at[:, :, his_cols], dres.at[:, own_rows], 0, partner)
    dres_msg.start()

    def comb(m, q):
        return remote(s_comb.at[m, q], r_comb.at[m, q], 1 + 2 * m + q, minus if m == 0 else plus)

    def dot_msg(q):
        return remote(dot_s.at[q], dot_r.at[q], 5 + q, partner)

    def spread(q, way):
        here = dxbuf.at[:, tok(chip, q), my_cols]
        return remote(here, here, 7 + 3 * q + way, (plus, minus, partner)[way])

    def far(q, m):
        here = dxbuf.at[m, tok(rel(3 if m == 0 else 1), q), my_cols]
        return remote(here, here, 13 + 2 * q + m, plus if m == 0 else minus)

    def near_fwd(q, side):
        here = dxbuf.at[:, tok(rel(3 if side == 0 else 1), q), my_cols]
        return remote(here, here, 17 + 2 * q + side, partner)

    def far_fwd(q, m):
        here = dxbuf.at[m, tok(rel(2), q), my_cols]
        return remote(here, here, 21 + 2 * q + m, partner)

    def dg_msg(way):
        return remote(dg_v, dg_r.at[way], 25 + way, (plus, minus, opposite)[way])

    dg_fin = remote(dg_half.at[0], dg_half.at[1], 28, partner)

    for cp in loads[:4]:
        cp.wait()
    for q in range(2):
        rows = slice(q * qrows, (q + 1) * qrows)
        s_comb[1, q] = keep[0, rows] + rp[0, rows]
        comb(1, q).start()
        s_comb[0, q] = keep[1, rows] + rm[0, rows]
        comb(0, q).start()
    for cp in loads[4:]:
        cp.wait()
    dres_msg.wait_recv()
    gain_half = gain_ref[:, my_cols].astype(F32)

    def hat_of(m, rows):
        xf = xc[m, rows].astype(F32)
        inv = lax.rsqrt(jnp.mean(xf * xf, axis=-1, keepdims=True) + NORM_EPS)
        return xc[m, rows, my_cols].astype(F32) * inv, inv

    def dn_finish(q):
        rows = slice(q * qrows, (q + 1) * qrows)
        part = jnp.zeros((1, half), F32)
        for m in range(2):
            comb(m, q).wait_recv()
            direct = rp[1, rows] if m == 0 else rm[1, rows]
            dn = keep[2 + m, rows] + direct + r_comb[m, q]
            dn_v[m, rows] = dn
            hat, _ = hat_of(m, rows)
            prod = dn * hat
            part = part + jnp.sum(prod, axis=0, keepdims=True)
            dots = jnp.sum(prod * gain_half, axis=-1, keepdims=True)
            dot_s[q, m] = jnp.broadcast_to(dots, (qrows, 128))
        dot_msg(q).start()
        if q == 0:
            dg_v[...] = part
        else:
            dg_v[...] += part
            for way in range(3):
                dg_msg(way).start()

    def dx_finish(q):
        rows = slice(q * qrows, (q + 1) * qrows)
        dot_msg(q).wait_recv()
        for m in range(2):
            hat, inv = hat_of(m, rows)
            centre = (dot_s[q, m, :, :1] + dot_r[q, m, :, :1]) * (1.0 / model_dim)
            dx = dres[m, rows].astype(F32) + inv * (gain_half * dn_v[m, rows] - hat * centre)
            dxbuf[m, tok(chip, q), my_cols] = dx.astype(BF16)
        for way in range(3):
            spread(q, way).start()

    def near_step(q):
        spread(q, 0).wait_recv()
        far(q, 0).start()
        near_fwd(q, 0).start()
        spread(q, 1).wait_recv()
        far(q, 1).start()
        near_fwd(q, 1).start()

    def dg_step():
        for way in range(3):
            dg_msg(way).wait_recv()
        dg_half[0] = dg_v[...] + dg_r[0] + dg_r[1] + dg_r[2]
        dg_fin.start()

    hooks = ((U_HOOKS[0], lambda: dn_finish(0)), (U_HOOKS[1], lambda: dx_finish(0)), (U_HOOKS[2], lambda: dn_finish(1)),
             (U_HOOKS[3], lambda: dx_finish(1)), (U_HOOKS[4], lambda: near_step(0)), (U_HOOKS[5], dg_step))

    def u_step(t, carry):
        @pl.when(t + 1 < steps)
        def _():
            w_copy(t + 1).start()

        w_copy(t).wait()

        @pl.when(t >= 2)
        def _():
            u_copy(t - 2).wait()

        slot = lax.rem(t, 2)
        ubuf[slot] = jnp.dot(n_v[...].reshape(total, model_dim), wbuf[slot], preferred_element_type=F32).astype(BF16).reshape(micro, seq_len, u_cols)
        u_copy(t).start()
        for at, hook in hooks:
            pl.when(t == at)(hook)
        return carry

    lax.fori_loop(0, steps, u_step, 0)
    near_step(1)
    for q in range(2):
        for m in range(2):
            far(q, m).wait_recv()
            far_fwd(q, m).start()
    dg_fin.wait_recv()
    dg_copies = [pltpu.make_async_copy(dg_half.at[0], dg_out.at[:, my_cols], osem.at[0]),
                 pltpu.make_async_copy(dg_half.at[1], dg_out.at[:, his_cols], osem.at[1])]
    for cp in dg_copies:
        cp.start()
    row_id = lax.broadcasted_iota(jnp.int32, (rows_loc, seq_len), 0) + dev * rows_loc
    hot = jnp.concatenate([jnp.where(row_id == ids_ref[m:m + 1, :], 1.0, 0.0).astype(BF16) for m in range(micro)], axis=1)
    for q in range(2):
        spread(q, 2).wait_recv()
        for side in range(2):
            near_fwd(q, side).wait_recv()
            far_fwd(q, side).wait_recv()
    de_steps = model_dim // DE_COLS

    def de_copy(i):
        cols = pl.ds(pl.multiple_of(i * DE_COLS, DE_COLS), DE_COLS)
        return pltpu.make_async_copy(de_v.at[:, cols], de_out.at[:, cols], osem.at[2 + i])

    def de_step(i, carry):
        cols = pl.ds(pl.multiple_of(i * DE_COLS, DE_COLS), DE_COLS)
        de_v[:, cols] = jnp.dot(hot, dxbuf[:, :, cols].reshape(total, DE_COLS), preferred_element_type=F32)
        de_copy(i).start()
        return carry

    lax.fori_loop(0, de_steps, de_step, 0)

    for i in range(de_steps):
        de_copy(i).wait()
    for cp in dg_copies:
        cp.wait()
    u_copy(steps - 2).wait()
    u_copy(steps - 1).wait()
    dres_msg.wait_send()
    dg_fin.wait_send()
    for way in range(3):
        dg_msg(way).wait_send()
    for q in range(2):
        dot_msg(q).wait_send()
        for m in range(2):
            comb(m, q).wait_send()
            far(q, m).wait_send()
            far_fwd(q, m).wait_send()
            near_fwd(q, m).wait_send()
        for way in range(3):
            spread(q, way).wait_send()


def finish_call(group, rows_loc, ids, gain2, rp, rm, keep, xchip, dres, n3, w):
    micro, seq_len = ids.shape
    model_dim, cols_loc = w.shape
    half = model_dim // 2
    chips = group // 2
    ctok = seq_len // chips
    qrows = ctok // 2
    total = micro * seq_len
    any_spec = pl.BlockSpec(memory_space=pl.ANY)
    vmem_spec = pl.BlockSpec(memory_space=pltpu.VMEM)
    return pl.pallas_call(
        functools.partial(finish_kernel, group),
        out_shape=(jax.ShapeDtypeStruct((micro, seq_len, cols_loc), BF16),
                   jax.ShapeDtypeStruct((rows_loc, model_dim), F32),
                   jax.ShapeDtypeStruct((1, model_dim), F32)),
        in_specs=[vmem_spec, vmem_spec] + [any_spec] * 7,
        out_specs=(any_spec,) * 3,
        scratch_shapes=[
            pltpu.VMEM((2, ctok, half), F32),
            pltpu.VMEM((2, ctok, half), F32),
            pltpu.VMEM((4, ctok, half), F32),
            pltpu.VMEM((micro, ctok, model_dim), BF16),
            pltpu.VMEM((micro, ctok, half), BF16),
            pltpu.VMEM((micro, seq_len, model_dim), BF16),
            pltpu.VMEM((2, model_dim, U_COLS), BF16),
            pltpu.VMEM((2, micro, seq_len, U_COLS), BF16),
            pltpu.VMEM((2, 2, qrows, half), F32),
            pltpu.VMEM((2, 2, qrows, half), F32),
            pltpu.VMEM((micro, ctok, half), F32),
            pltpu.VMEM((2, micro, qrows, 128), F32),
            pltpu.VMEM((2, micro, qrows, 128), F32),
            pltpu.VMEM((micro, seq_len, model_dim), BF16),
            pltpu.VMEM((1, half), F32),
            pltpu.VMEM((3, 1, half), F32),
            pltpu.VMEM((2, 1, half), F32),
            pltpu.VMEM((rows_loc, model_dim), F32),
            pltpu.SemaphoreType.DMA((6,)),
            pltpu.SemaphoreType.DMA((2,)),
            pltpu.SemaphoreType.DMA((2,)),
            pltpu.SemaphoreType.DMA((2 + model_dim // DE_COLS,)),
            pltpu.SemaphoreType.DMA((29,)),
            pltpu.SemaphoreType.DMA((29,)),
        ],
        compiler_params=pltpu.CompilerParams(collective_id=1, has_side_effects=True, vmem_limit_bytes=58 * 1024 * 1024),
        cost_estimate=pl.CostEstimate(flops=2 * total * cols_loc * model_dim, bytes_accessed=2 * cols_loc * model_dim, transcendentals=0),
        name="finish_u",
    )(ids, gain2, rp, rm, keep, xchip, dres, n3, w)


def solution(mesh):
    group = mesh.shape['tp']
    plus = [(r, (r + 2) % group) for r in range(group)]
    minus = [(r, (r - 2) % group) for r in range(group)]

    def local_step(token_ids, table_loc, gain_vec, w_loc, du_loc, dres_loc):
        micro, seq_len = token_ids.shape
        model_dim, cols_loc = w_loc.shape
        own_tok = dres_loc.shape[1]
        total = micro * seq_len
        core = lax.rem(lax.axis_index('tp'), 2)
        gain2 = gain_vec.reshape(1, model_dim)
        normed, x_chip, msg_plus, msg_minus, keep = gather_call(group, token_ids, gain2, table_loc, w_loc, du_loc)
        got_plus = lax.ppermute(msg_plus, 'tp', plus)
        got_minus = lax.ppermute(msg_minus, 'tp', minus)
        grad_w = weight_grad_call(normed.reshape(total, model_dim), du_loc.reshape(total, cols_loc))
        u, grad_table, grad_gain = finish_call(group, table_loc.shape[0], token_ids, gain2, got_plus, got_minus, keep, x_chip, dres_loc, normed, w_loc)
        x_own = lax.dynamic_slice_in_dim(x_chip, core * own_tok, own_tok, axis=1)
        return u, x_own, grad_table, grad_w, grad_gain.reshape(model_dim)

    return jax.shard_map(local_step, mesh=mesh,
                         in_specs=(P('dp', None), P('tp', None), P(None), P(None, 'tp'), P('dp', None, 'tp'), P('dp', 'tp', None)),
                         out_specs=(P('dp', None, 'tp'), P('dp', 'tp', None), P(('dp', 'tp'), None), P(None, ('dp', 'tp')), P('dp')),
                         check_vma=False)
```

```python
import functools

import jax
import jax.numpy as jnp
from jax import lax
from jax.experimental import pallas as pl
from jax.experimental.pallas import tpu as pltpu
from jax.sharding import PartitionSpec as P

NORM_EPS = 1e-6
MESH = pl.DeviceIdType.MESH
F32 = jnp.float32
BF16 = jnp.bfloat16
DN_TILE = 256
RELAY_AT = (3, 5)
SUM_AT = (10, 12)
DW_ROWS = 896
DW_COLS = 1536
U_COLS = 256
U_HOOKS = (5, 7, 10, 12, 17, 15)
DE_COLS = 512
U_PARTS = 4


def gather_kernel(group, ids_ref, gain_ref, table_ref, w_ref, du_ref,
                  n_out, xchip_out, plus_out, minus_out, keep_out,
                  tab, looked, r_relay, r_direct, r_comb, s_comb, xbuf, n_v, du_v, wbuf, dn2, dnp, stage,
                  lsem, wsem, osem, snd, rcv):
    dev = lax.axis_index('tp')
    chips = group // 2
    chip = lax.div(dev, 2)
    core = lax.rem(dev, 2)
    plus = lax.rem(dev + 2, group)
    minus = lax.rem(dev + group - 2, group)
    partner = dev + 1 - 2 * core
    micro, seq_len = ids_ref.shape
    rows_loc, model_dim = table_ref.shape
    half = model_dim // 2
    ctok = seq_len // chips
    qrows = ctok // 2
    tiles = half // DN_TILE
    my_cols = pl.ds(pl.multiple_of(core * half, 128), half)
    his_cols = pl.ds(pl.multiple_of((1 - core) * half, 128), half)

    def rel(j):
        return lax.rem(chip + j, chips)

    def tok(d, q=None):
        if q is None:
            return pl.ds(pl.multiple_of(d * ctok, ctok), ctok)
        return pl.ds(pl.multiple_of(d * ctok + q * qrows, qrows), qrows)

    def remote(src, dst, slot, target):
        return pltpu.make_async_remote_copy(src_ref=src, dst_ref=dst, send_sem=snd.at[slot], recv_sem=rcv.at[slot],
                                            device_id={'tp': target}, device_id_type=MESH)

    cp_du = pltpu.make_async_copy(du_ref, du_v, lsem.at[0])
    cp_tab = pltpu.make_async_copy(table_ref.at[:, my_cols],
                                   tab.at[pl.ds(pl.multiple_of(core * rows_loc, rows_loc), rows_loc)], lsem.at[1])

    def w_copy(t):
        ft = jnp.where(t < tiles, (1 - core) * tiles + t, core * tiles + t - tiles)
        slot = lax.rem(t, 2)
        return pltpu.make_async_copy(w_ref.at[pl.ds(pl.multiple_of(ft * DN_TILE, DN_TILE), DN_TILE), :], wbuf.at[slot],
                                     wsem.at[slot])

    cp_tab.start()
    cp_du.start()
    w_copy(0).start()

    barrier = pltpu.get_barrier_semaphore()
    for target in (plus, minus, partner):
        pl.semaphore_signal(barrier, inc=1, device_id={'tp': target}, device_id_type=MESH)
    pl.semaphore_wait(barrier, 3)

    table_msg = remote(table_ref.at[:, his_cols], tab.at[pl.ds(pl.multiple_of(core * rows_loc, rows_loc), rows_loc)], 0, partner)
    table_msg.start()

    def relay(m, q):
        return remote(looked.at[m, tok(rel(2), q)], r_relay.at[m, q], 1 + 2 * m + q, minus if m == 0 else plus)

    def direct(m, q):
        return remote(looked.at[m, tok(rel(1 if m == 0 else 3), q)], r_direct.at[m, q], 5 + 2 * m + q, plus if m == 0 else minus)

    def comb(m, q):
        return remote(s_comb.at[m, q], r_comb.at[m, q], 9 + 2 * m + q, minus if m == 0 else plus)

    def spread(q, way):
        here = xbuf.at[:, tok(chip, q), my_cols]
        return remote(here, here, 13 + 3 * q + way, (plus, minus, partner)[way])

    def far(q, m):
        here = xbuf.at[m, tok(rel(3 if m == 0 else 1), q), my_cols]
        return remote(here, here, 19 + 2 * q + m, plus if m == 0 else minus)

    def near_fwd(q, side):
        here = xbuf.at[:, tok(rel(3 if side == 0 else 1), q), my_cols]
        return remote(here, here, 23 + 2 * q + side, partner)

    def far_fwd(q, m):
        here = xbuf.at[m, tok(rel(2), q), my_cols]
        return remote(here, here, 27 + 2 * q + m, partner)

    def dn_msg(t):
        cols = pl.ds(pl.multiple_of(t * DN_TILE, DN_TILE), DN_TILE)
        return remote(dn2.at[0, :, :, cols], dnp.at[:, :, cols], 31 + t, partner)

    cp_tab.wait()
    table_msg.wait_recv()
    row_id = lax.broadcasted_iota(jnp.int32, (2 * rows_loc, seq_len), 0) + chip * (2 * rows_loc)
    for m in (1, 0):
        hot = jnp.where(row_id == ids_ref[m:m + 1, :], 1.0, 0.0).astype(BF16)
        looked[m] = lax.dot_general(hot, tab[...], (((0,), (0,)), ((), ())), preferred_element_type=F32).astype(BF16)
    for q in range(2):
        for m in range(2):
            relay(m, q).start()
    for q in range(2):
        for m in range(2):
            direct(m, q).start()
    cp_du.wait()

    def relay_step(q):
        for m in range(2):
            relay(m, q).wait_recv()
            s_comb[m, q] = looked[m, tok(rel(3 if m == 0 else 1), q)] + r_relay[m, q]
            comb(m, q).start()

    def sum_step(q):
        for m in range(2):
            direct(m, q).wait_recv()
            comb(m, q).wait_recv()
            xbuf[m, tok(chip, q), my_cols] = (looked[m, tok(chip, q)] + r_direct[m, q]) + r_comb[m, q]
        for way in range(3):
            spread(q, way).start()

    def dn_step(t, carry):
        @pl.when(t + 1 < 2 * tiles)
        def _():
            w_copy(t + 1).start()

        w_copy(t).wait()
        slot = lax.rem(t, 2)
        part = lax.dot_general(du_v[...].reshape(micro * seq_len, du_v.shape[2]), wbuf[slot], (((1,), (1,)), ((), ())),
                               preferred_element_type=F32).astype(BF16).reshape(micro, seq_len, DN_TILE)
        side = lax.div(t, tiles)
        col = (t - side * tiles) * DN_TILE
        dn2[side, :, :, pl.ds(pl.multiple_of(col, DN_TILE), DN_TILE)] = part

        @pl.when(t < tiles)
        def _():
            dn_msg(t).start()

        for q in range(2):
            @pl.when(t == RELAY_AT[q])
            def _():
                relay_step(q)
        for q in range(2):
            @pl.when(t == SUM_AT[q])
            def _():
                sum_step(q)
        return carry

    lax.fori_loop(0, 2 * tiles, dn_step, 0)

    def dn_wait(t, carry):
        dn_msg(t).wait_recv()
        return carry

    lax.fori_loop(0, tiles, dn_wait, 0)

    terms = ((2, 1), (1, 0), (2, 0), (3, 1), (1, 1), (3, 0), (0, 0), (0, 1))

    def s_copy(i):
        out = (plus_out, minus_out, keep_out, keep_out)[i // 2]
        return pltpu.make_async_copy(stage.at[i], out.at[i % 2 if i < 4 else i - 4], osem.at[i])

    def s_steps():
        for i, (j, m) in enumerate(terms):
            stage[i] = dn2[1, m, tok(rel(j))].astype(F32) + dnp[m, tok(rel(j))].astype(F32)
            s_copy(i).start()

    def near_step(q):
        spread(q, 0).wait_recv()
        far(q, 0).start()
        near_fwd(q, 0).start()
        spread(q, 1).wait_recv()
        far(q, 1).start()
        near_fwd(q, 1).start()

    near_step(0)
    s_steps()
    near_step(1)

    def n_copy(d, i):
        return pltpu.make_async_copy(n_v.at[:, tok(d)], n_out.at[:, tok(d)], osem.at[2 * chips + i])

    gain_f = gain_ref[...].astype(F32).reshape(1, model_dim)

    def norm_piece(j):
        d = rel(j)

        def body(i, carry):
            m, r = lax.div(i, ctok // 16), lax.rem(i, ctok // 16)
            rows = pl.ds(pl.multiple_of(d * ctok + r * 16, 16), 16)
            xf = xbuf[m, rows].astype(F32)
            inv = lax.rsqrt(jnp.mean(xf * xf, axis=-1, keepdims=True) + NORM_EPS)
            n_v[m, rows] = (xf * inv * gain_f).astype(BF16)
            return carry

        lax.fori_loop(0, micro * (ctok // 16), body, 0)
        n_copy(d, j).start()

    for q in range(2):
        spread(q, 2).wait_recv()
    cp_x = pltpu.make_async_copy(xbuf.at[:, tok(chip)], xchip_out, lsem.at[0])
    cp_x.start()
    norm_piece(0)
    for q in range(2):
        for m in range(2):
            far(q, m).wait_recv()
            far_fwd(q, m).start()
    for side, j in ((0, 3), (1, 1)):
        for q in range(2):
            near_fwd(q, side).wait_recv()
        norm_piece(j)
    for q in range(2):
        for m in range(2):
            far_fwd(q, m).wait_recv()
    norm_piece(2)

    for i in range(2 * chips):
        s_copy(i).wait()
    for j in range(chips):
        n_copy(rel(j), j).wait()
    cp_x.wait()
    table_msg.wait_send()
    for q in range(2):
        for m in range(2):
            relay(m, q).wait_send()
            direct(m, q).wait_send()
            comb(m, q).wait_send()
            far(q, m).wait_send()
            far_fwd(q, m).wait_send()
            near_fwd(q, m).wait_send()
        for way in range(3):
            spread(q, way).wait_send()

    def dn_drain(t, carry):
        dn_msg(t).wait_send()
        return carry

    lax.fori_loop(0, tiles, dn_drain, 0)


def gather_call(group, ids, gain2, table, w, du):
    micro, seq_len = ids.shape
    rows_loc, model_dim = table.shape
    cols_loc = w.shape[1]
    half = model_dim // 2
    chips = group // 2
    ctok = seq_len // chips
    tiles = half // DN_TILE
    hbm_spec = pl.BlockSpec(memory_space=pltpu.HBM)
    vmem_spec = pl.BlockSpec(memory_space=pltpu.VMEM)
    msg = pltpu.VMEM((2, 2, ctok // 2, half), BF16)
    total = micro * seq_len
    return pl.pallas_call(
        functools.partial(gather_kernel, group),
        out_shape=(jax.ShapeDtypeStruct((micro, seq_len, model_dim), BF16),
                   jax.ShapeDtypeStruct((micro, ctok, model_dim), BF16),
                   jax.ShapeDtypeStruct((2, ctok, half), F32),
                   jax.ShapeDtypeStruct((2, ctok, half), F32),
                   jax.ShapeDtypeStruct((4, ctok, half), F32)),
        in_specs=[vmem_spec, vmem_spec, hbm_spec, hbm_spec, hbm_spec],
        out_specs=(hbm_spec,) * 5,
        scratch_shapes=[
            pltpu.VMEM((2 * rows_loc, half), BF16),
            pltpu.VMEM((micro, seq_len, half), BF16),
            msg, msg, msg, msg,
            pltpu.VMEM((micro, seq_len, model_dim), BF16),
            pltpu.VMEM((micro, seq_len, model_dim), BF16),
            pltpu.VMEM((micro, seq_len, cols_loc), BF16),
            pltpu.VMEM((2, DN_TILE, cols_loc), BF16),
            pltpu.VMEM((2, micro, seq_len, half), BF16),
            pltpu.VMEM((micro, seq_len, half), BF16),
            pltpu.VMEM((2 * chips, ctok, half), F32),
            pltpu.SemaphoreType.DMA((2,)),
            pltpu.SemaphoreType.DMA((2,)),
            pltpu.SemaphoreType.DMA((3 * chips,)),
            pltpu.SemaphoreType.DMA((31 + tiles,)),
            pltpu.SemaphoreType.DMA((31 + tiles,)),
        ],
        compiler_params=pltpu.CompilerParams(collective_id=0, has_side_effects=True, vmem_limit_bytes=58 * 1024 * 1024),
        cost_estimate=pl.CostEstimate(flops=2 * total * cols_loc * model_dim, bytes_accessed=2 * cols_loc * model_dim, transcendentals=0),
        name="gather_dn",
    )(ids, gain2, table, w, du)


def weight_grad_kernel(n_ref, du_ref, out_ref):
    cols = pl.ds(pl.multiple_of(pl.program_id(1) * DW_COLS, DW_COLS), DW_COLS)
    out_ref[...] = lax.dot_general(n_ref[...], du_ref[:, cols], (((0,), (0,)), ((), ())), preferred_element_type=F32)


def weight_grad_call(n2, du2):
    total, model_dim = n2.shape
    cols = du2.shape[1]
    return pl.pallas_call(
        weight_grad_kernel,
        grid=(model_dim // DW_ROWS, cols // DW_COLS),
        out_shape=jax.ShapeDtypeStruct((model_dim, cols), F32),
        in_specs=[pl.BlockSpec((total, DW_ROWS), lambda i, j: (0, i)), pl.BlockSpec((total, cols), lambda i, j: (0, 0))],
        out_specs=pl.BlockSpec((DW_ROWS, DW_COLS), lambda i, j: (i, j)),
        compiler_params=pltpu.CompilerParams(dimension_semantics=("arbitrary", "arbitrary"), vmem_limit_bytes=63 * 1024 * 1024),
        cost_estimate=pl.CostEstimate(flops=2 * total * cols * model_dim, bytes_accessed=4 * cols * model_dim, transcendentals=0),
        name="weight_grad",
    )(n2, du2)


def finish_kernel(group, ids_ref, gain_ref, rp_ref, rm_ref, keep_ref, xchip_ref, dres_ref, n_ref, w_ref,
                  u_out, dx_out, dg_out,
                  rp, rm, keep, xc, dres, n_v, wbuf, ubuf, s_comb, r_comb, dn_v, dot_s, dot_r, dxbuf, dg_v, dg_r, dg_half,
                  lsem, wsem, usem, osem, snd, rcv):
    dev = lax.axis_index('tp')
    chips = group // 2
    chip = lax.div(dev, 2)
    core = lax.rem(dev, 2)
    plus = lax.rem(dev + 2, group)
    minus = lax.rem(dev + group - 2, group)
    opposite = lax.rem(dev + group // 2, group)
    partner = dev + 1 - 2 * core
    micro, seq_len = ids_ref.shape
    model_dim = gain_ref.shape[0]
    half = model_dim // 2
    ctok = seq_len // chips
    qrows = ctok // 2
    u_cols = wbuf.shape[2]
    steps = w_ref.shape[1] // u_cols
    total = micro * seq_len
    my_cols = pl.ds(pl.multiple_of(core * half, 128), half)
    his_cols = pl.ds(pl.multiple_of((1 - core) * half, 128), half)

    def rel(j):
        return lax.rem(chip + j, chips)

    def tok(d, q=None):
        if q is None:
            return pl.ds(pl.multiple_of(d * ctok, ctok), ctok)
        return pl.ds(pl.multiple_of(d * ctok + q * qrows, qrows), qrows)

    def remote(src, dst, slot, target):
        return pltpu.make_async_remote_copy(src_ref=src, dst_ref=dst, send_sem=snd.at[slot], recv_sem=rcv.at[slot],
                                            device_id={'tp': target}, device_id_type=MESH)

    def local(src, dst, i):
        return pltpu.make_async_copy(src, dst, lsem.at[i])

    own_rows = pl.ds(pl.multiple_of(core * qrows, qrows), qrows)
    loads = [local(rp_ref, rp, 0), local(rm_ref, rm, 1), local(keep_ref, keep, 2), local(xchip_ref, xc, 3),
             local(n_ref, n_v, 4), local(dres_ref.at[:, :, my_cols], dres.at[:, own_rows], 5)]
    for cp in loads[:4]:
        cp.start()

    def w_copy(t):
        slot = lax.rem(t, 2)
        return pltpu.make_async_copy(w_ref.at[:, pl.ds(pl.multiple_of(t * u_cols, u_cols), u_cols)], wbuf.at[slot], wsem.at[slot])

    def u_copy(t):
        slot = lax.rem(t, 2)
        return pltpu.make_async_copy(ubuf.at[slot], u_out.at[:, :, pl.ds(pl.multiple_of(t * u_cols, u_cols), u_cols)], usem.at[slot])

    loads[4].start()
    loads[5].start()
    w_copy(0).start()

    barrier = pltpu.get_barrier_semaphore()
    for target in (plus, minus, partner, opposite):
        pl.semaphore_signal(barrier, inc=1, device_id={'tp': target}, device_id_type=MESH)
    pl.semaphore_wait(barrier, 4)

    dres_msg = remote(dres_ref.at[:, :, his_cols], dres.at[:, own_rows], 0, partner)
    dres_msg.start()

    def comb(m, q):
        return remote(s_comb.at[m, q], r_comb.at[m, q], 1 + 2 * m + q, minus if m == 0 else plus)

    def dot_msg(q):
        return remote(dot_s.at[q], dot_r.at[q], 5 + q, partner)

    def spread(q, way):
        here = dxbuf.at[:, tok(chip, q), my_cols]
        return remote(here, here, 7 + 3 * q + way, (plus, minus, partner)[way])

    def far(q, m):
        here = dxbuf.at[m, tok(rel(3 if m == 0 else 1), q), my_cols]
        return remote(here, here, 13 + 2 * q + m, plus if m == 0 else minus)

    def near_fwd(q, side):
        here = dxbuf.at[:, tok(rel(3 if side == 0 else 1), q), my_cols]
        return remote(here, here, 17 + 2 * q + side, partner)

    def far_fwd(q, m):
        here = dxbuf.at[m, tok(rel(2), q), my_cols]
        return remote(here, here, 21 + 2 * q + m, partner)

    def dg_msg(way):
        return remote(dg_v, dg_r.at[way], 25 + way, (plus, minus, opposite)[way])

    dg_fin = remote(dg_half.at[0], dg_half.at[1], 28, partner)

    for cp in loads[:4]:
        cp.wait()
    for q in range(2):
        rows = slice(q * qrows, (q + 1) * qrows)
        s_comb[1, q] = keep[0, rows] + rp[0, rows]
        comb(1, q).start()
        s_comb[0, q] = keep[1, rows] + rm[0, rows]
        comb(0, q).start()
    for cp in loads[4:]:
        cp.wait()
    dres_msg.wait_recv()
    gain_half = gain_ref[my_cols].astype(F32).reshape(1, half)

    def hat_of(m, rows):
        xf = xc[m, rows].astype(F32)
        inv = lax.rsqrt(jnp.mean(xf * xf, axis=-1, keepdims=True) + NORM_EPS)
        return xc[m, rows, my_cols].astype(F32) * inv, inv

    def dn_finish(q):
        rows = slice(q * qrows, (q + 1) * qrows)
        part = jnp.zeros((1, half), F32)
        for m in range(2):
            comb(m, q).wait_recv()
            direct = rp[1, rows] if m == 0 else rm[1, rows]
            dn = keep[2 + m, rows] + direct + r_comb[m, q]
            dn_v[m, rows] = dn
            hat, _ = hat_of(m, rows)
            prod = dn * hat
            part = part + jnp.sum(prod, axis=0, keepdims=True)
            dots = jnp.sum(prod * gain_half, axis=-1, keepdims=True)
            dot_s[q, m] = jnp.broadcast_to(dots, (qrows, 128))
        dot_msg(q).start()
        if q == 0:
            dg_v[...] = part
        else:
            dg_v[...] += part
            for way in range(3):
                dg_msg(way).start()

    def dx_finish(q):
        rows = slice(q * qrows, (q + 1) * qrows)
        dot_msg(q).wait_recv()
        for m in range(2):
            hat, inv = hat_of(m, rows)
            centre = (dot_s[q, m, :, :1] + dot_r[q, m, :, :1]) * (1.0 / model_dim)
            dx = dres[m, rows].astype(F32) + inv * (gain_half * dn_v[m, rows] - hat * centre)
            dxbuf[m, tok(chip, q), my_cols] = dx.astype(BF16)
        for way in range(3):
            spread(q, way).start()

    def near_step(q):
        spread(q, 0).wait_recv()
        far(q, 0).start()
        near_fwd(q, 0).start()
        spread(q, 1).wait_recv()
        far(q, 1).start()
        near_fwd(q, 1).start()

    def dg_step():
        for way in range(3):
            dg_msg(way).wait_recv()
        dg_half[0] = dg_v[...] + dg_r[0] + dg_r[1] + dg_r[2]
        dg_fin.start()

    hooks = ((U_HOOKS[0], lambda: dn_finish(0)), (U_HOOKS[1], lambda: dx_finish(0)), (U_HOOKS[2], lambda: dn_finish(1)),
             (U_HOOKS[3], lambda: dx_finish(1)), (U_HOOKS[4], lambda: near_step(0)), (U_HOOKS[5], dg_step))

    def u_step(t, carry):
        @pl.when(t + 1 < steps)
        def _():
            w_copy(t + 1).start()

        w_copy(t).wait()

        @pl.when(t >= 2)
        def _():
            u_copy(t - 2).wait()

        slot = lax.rem(t, 2)
        ubuf[slot] = jnp.dot(n_v[...].reshape(total, model_dim), wbuf[slot], preferred_element_type=F32).astype(BF16).reshape(micro, seq_len, u_cols)
        u_copy(t).start()
        for at, hook in hooks:
            pl.when(t == at)(hook)
        return carry

    lax.fori_loop(0, steps, u_step, 0)
    near_step(1)
    for q in range(2):
        for m in range(2):
            far(q, m).wait_recv()
            far_fwd(q, m).start()
    dg_fin.wait_recv()
    dg_copies = [pltpu.make_async_copy(dg_half.at[0], dg_out.at[:, my_cols], osem.at[0]),
                 pltpu.make_async_copy(dg_half.at[1], dg_out.at[:, his_cols], osem.at[1])]
    for cp in dg_copies:
        cp.start()
    for q in range(2):
        spread(q, 2).wait_recv()
        for side in range(2):
            near_fwd(q, side).wait_recv()
    near_copies = [pltpu.make_async_copy(dxbuf.at[:, tok(rel(j))], dx_out.at[:, tok(rel(j))], osem.at[2 + j]) for j in range(chips)]
    for j in (0, 1, 3):
        near_copies[j].start()
    for q in range(2):
        for side in range(2):
            far_fwd(q, side).wait_recv()
    near_copies[2].start()

    for cp in near_copies:
        cp.wait()
    for cp in dg_copies:
        cp.wait()
    u_copy(steps - 2).wait()
    u_copy(steps - 1).wait()
    dres_msg.wait_send()
    dg_fin.wait_send()
    for way in range(3):
        dg_msg(way).wait_send()
    for q in range(2):
        dot_msg(q).wait_send()
        for m in range(2):
            comb(m, q).wait_send()
            far(q, m).wait_send()
            far_fwd(q, m).wait_send()
            near_fwd(q, m).wait_send()
        for way in range(3):
            spread(q, way).wait_send()


def finish_call(group, ids, gain2, rp, rm, keep, xchip, dres, n3, w):
    micro, seq_len = ids.shape
    model_dim, cols_loc = w.shape
    half = model_dim // 2
    chips = group // 2
    ctok = seq_len // chips
    qrows = ctok // 2
    total = micro * seq_len
    hbm_spec = pl.BlockSpec(memory_space=pltpu.HBM)
    any_spec = pl.BlockSpec(memory_space=pl.ANY)
    vmem_spec = pl.BlockSpec(memory_space=pltpu.VMEM)
    return pl.pallas_call(
        functools.partial(finish_kernel, group),
        out_shape=(jax.ShapeDtypeStruct((micro, seq_len, cols_loc), BF16),
                   jax.ShapeDtypeStruct((micro, seq_len, model_dim), BF16),
                   jax.ShapeDtypeStruct((1, model_dim), F32)),
        in_specs=[vmem_spec, vmem_spec] + [hbm_spec] * 7,
        out_specs=(any_spec,) * 3,
        scratch_shapes=[
            pltpu.VMEM((2, ctok, half), F32),
            pltpu.VMEM((2, ctok, half), F32),
            pltpu.VMEM((4, ctok, half), F32),
            pltpu.VMEM((micro, ctok, model_dim), BF16),
            pltpu.VMEM((micro, ctok, half), BF16),
            pltpu.VMEM((micro, seq_len, model_dim), BF16),
            pltpu.VMEM((2, model_dim, U_COLS), BF16),
            pltpu.VMEM((2, micro, seq_len, U_COLS), BF16),
            pltpu.VMEM((2, 2, qrows, half), F32),
            pltpu.VMEM((2, 2, qrows, half), F32),
            pltpu.VMEM((micro, ctok, half), F32),
            pltpu.VMEM((2, micro, qrows, 128), F32),
            pltpu.VMEM((2, micro, qrows, 128), F32),
            pltpu.VMEM((micro, seq_len, model_dim), BF16),
            pltpu.VMEM((1, half), F32),
            pltpu.VMEM((3, 1, half), F32),
            pltpu.VMEM((2, 1, half), F32),
            pltpu.SemaphoreType.DMA((6,)),
            pltpu.SemaphoreType.DMA((2,)),
            pltpu.SemaphoreType.DMA((2,)),
            pltpu.SemaphoreType.DMA((2 + chips,)),
            pltpu.SemaphoreType.DMA((29,)),
            pltpu.SemaphoreType.DMA((29,)),
        ],
        compiler_params=pltpu.CompilerParams(collective_id=1, has_side_effects=True, vmem_limit_bytes=30 * 1024 * 1024),
        cost_estimate=pl.CostEstimate(flops=2 * total * cols_loc * model_dim, bytes_accessed=2 * cols_loc * model_dim, transcendentals=0),
        name="finish_u",
    )(ids, gain2, rp, rm, keep, xchip, dres, n3, w)


def epilogue_kernel(ids_ref, u_ref, dx_ref, dg_ref, u_out, de_out, dg_out, u_v, dx_v, de_v, usem, xsem):
    dev = lax.axis_index('tp')
    micro, seq_len = ids_ref.shape
    rows_loc, model_dim = de_v.shape
    steps = model_dim // DE_COLS
    ucols = u_v.shape[2] // U_PARTS

    def cols(i, n):
        return pl.ds(i * n, n)

    x_loads = [pltpu.make_async_copy(dx_ref.at[:, :, cols(i, DE_COLS)], dx_v.at[:, :, cols(i, DE_COLS)], xsem.at[i]) for i in range(steps)]
    u_loads = [pltpu.make_async_copy(u_ref.at[:, :, cols(i, ucols)], u_v.at[:, :, cols(i, ucols)], usem.at[i]) for i in range(U_PARTS)]
    x_loads[0].start()
    x_loads[1].start()
    for cp in u_loads:
        cp.start()
    for cp in x_loads[2:]:
        cp.start()
    dg_out[...] = dg_ref[0]
    row_id = lax.broadcasted_iota(jnp.int32, (rows_loc, seq_len), 0) + dev * rows_loc
    hot = jnp.concatenate([jnp.where(row_id == ids_ref[m:m + 1, :], 1.0, 0.0).astype(BF16) for m in range(micro)], axis=1)
    u_stores = [pltpu.make_async_copy(u_v.at[:, :, cols(i, ucols)], u_out.at[:, :, cols(i, ucols)], usem.at[U_PARTS + i]) for i in range(U_PARTS)]
    de_stores = [pltpu.make_async_copy(de_v.at[:, cols(i, DE_COLS)], de_out.at[:, cols(i, DE_COLS)], xsem.at[steps + i]) for i in range(steps)]
    for i in range(steps):
        x_loads[i].wait()
        de_v[:, cols(i, DE_COLS)] = jnp.dot(hot, dx_v[:, :, cols(i, DE_COLS)].reshape(micro * seq_len, DE_COLS), preferred_element_type=F32)
        de_stores[i].start()
        if i < U_PARTS:
            u_loads[i].wait()
            u_stores[i].start()
    for cp in u_stores + de_stores:
        cp.wait()


def epilogue_call(rows_loc, ids, u, dx, dg):
    micro, seq_len, _ = u.shape
    model_dim = dx.shape[2]
    steps = model_dim // DE_COLS
    any_spec = pl.BlockSpec(memory_space=pl.ANY)
    vmem_spec = pl.BlockSpec(memory_space=pltpu.VMEM)
    return pl.pallas_call(
        epilogue_kernel,
        out_shape=(jax.ShapeDtypeStruct(u.shape, BF16), jax.ShapeDtypeStruct((rows_loc, model_dim), F32),
                   jax.ShapeDtypeStruct((model_dim,), F32)),
        in_specs=[vmem_spec, any_spec, any_spec, vmem_spec],
        out_specs=(any_spec, any_spec, vmem_spec),
        scratch_shapes=[
            pltpu.VMEM(u.shape, BF16),
            pltpu.VMEM(dx.shape, BF16),
            pltpu.VMEM((rows_loc, model_dim), F32),
            pltpu.SemaphoreType.DMA((2 * U_PARTS,)),
            pltpu.SemaphoreType.DMA((2 * steps,)),
        ],
        compiler_params=pltpu.CompilerParams(vmem_limit_bytes=22 * 1024 * 1024),
        cost_estimate=pl.CostEstimate(flops=2 * micro * seq_len * rows_loc * model_dim, bytes_accessed=4 * rows_loc * model_dim, transcendentals=0),
        name="epilogue",
    )(ids, u, dx, dg)


def solution(mesh):
    group = mesh.shape['tp']
    plus = [(r, (r + 2) % group) for r in range(group)]
    minus = [(r, (r - 2) % group) for r in range(group)]

    def local_step(token_ids, table_loc, gain_vec, w_loc, du_loc, dres_loc):
        micro, seq_len = token_ids.shape
        model_dim, cols_loc = w_loc.shape
        own_tok = dres_loc.shape[1]
        total = micro * seq_len
        core = lax.rem(lax.axis_index('tp'), 2)
        gain2 = gain_vec
        normed, x_chip, msg_plus, msg_minus, keep = gather_call(group, token_ids, gain2, table_loc, w_loc, du_loc)
        got_plus = lax.ppermute(msg_plus, 'tp', plus)
        got_minus = lax.ppermute(msg_minus, 'tp', minus)
        grad_w = weight_grad_call(normed.reshape(total, model_dim), du_loc.reshape(total, cols_loc))
        u_tmp, dx_all, dg = finish_call(group, token_ids, gain2, got_plus, got_minus, keep, x_chip, dres_loc, normed, w_loc)
        u, grad_table, grad_gain = epilogue_call(table_loc.shape[0], token_ids, u_tmp, dx_all, dg)
        x_own = lax.dynamic_slice_in_dim(x_chip, core * own_tok, own_tok, axis=1)
        return u, x_own, grad_table, grad_w, grad_gain

    return jax.shard_map(local_step, mesh=mesh,
                         in_specs=(P('dp', None), P('tp', None), P(None), P(None, 'tp'), P('dp', None, 'tp'), P('dp', 'tp', None)),
                         out_specs=(P('dp', None, 'tp'), P('dp', 'tp', None), P(('dp', 'tp'), None), P(None, ('dp', 'tp')), P('dp')),
                         check_vma=False)
```

```python
import functools

import jax
import jax.numpy as jnp
from jax import lax
from jax.experimental import pallas as pl
from jax.experimental.pallas import tpu as pltpu
from jax.sharding import PartitionSpec as P

NORM_EPS = 1e-6
MESH = pl.DeviceIdType.MESH
F32 = jnp.float32
BF16 = jnp.bfloat16
DN_TILE = 256
RELAY_AT = (3, 5)
SUM_AT = (10, 12)
DW_ROWS = 256
DW_COLS = 2304
DW_SLOTS = 6
U_COLS = 256
U_HOOKS = (5, 7, 10, 12, 17, 15)
DE_COLS = 512
U_PARTS = 4


def gather_kernel(group, ids_ref, gain_ref, table_ref, w_ref, du_ref,
                  n_out, xchip_out, plus_out, minus_out, keep_out,
                  tab, looked, r_relay, r_direct, r_comb, s_comb, xbuf, n_v, du_v, wbuf, dn2, dnp, stage,
                  lsem, wsem, osem, snd, rcv):
    dev = lax.axis_index('tp')
    chips = group // 2
    chip = lax.div(dev, 2)
    core = lax.rem(dev, 2)
    plus = lax.rem(dev + 2, group)
    minus = lax.rem(dev + group - 2, group)
    partner = dev + 1 - 2 * core
    micro, seq_len = ids_ref.shape
    rows_loc, model_dim = table_ref.shape
    half = model_dim // 2
    ctok = seq_len // chips
    qrows = ctok // 2
    tiles = half // DN_TILE
    my_cols = pl.ds(pl.multiple_of(core * half, 128), half)
    his_cols = pl.ds(pl.multiple_of((1 - core) * half, 128), half)

    def rel(j):
        return lax.rem(chip + j, chips)

    def tok(d, q=None):
        if q is None:
            return pl.ds(pl.multiple_of(d * ctok, ctok), ctok)
        return pl.ds(pl.multiple_of(d * ctok + q * qrows, qrows), qrows)

    def remote(src, dst, slot, target):
        return pltpu.make_async_remote_copy(src_ref=src, dst_ref=dst, send_sem=snd.at[slot], recv_sem=rcv.at[slot],
                                            device_id={'tp': target}, device_id_type=MESH)

    cp_du = pltpu.make_async_copy(du_ref, du_v, lsem.at[0])
    cp_tab = pltpu.make_async_copy(table_ref.at[:, my_cols],
                                   tab.at[pl.ds(pl.multiple_of(core * rows_loc, rows_loc), rows_loc)], lsem.at[1])

    def w_copy(t):
        ft = jnp.where(t < tiles, (1 - core) * tiles + t, core * tiles + t - tiles)
        slot = lax.rem(t, 2)
        return pltpu.make_async_copy(w_ref.at[pl.ds(pl.multiple_of(ft * DN_TILE, DN_TILE), DN_TILE), :], wbuf.at[slot],
                                     wsem.at[slot])

    cp_tab.start()
    cp_du.start()
    w_copy(0).start()

    barrier = pltpu.get_barrier_semaphore()
    for target in (plus, minus, partner):
        pl.semaphore_signal(barrier, inc=1, device_id={'tp': target}, device_id_type=MESH)
    pl.semaphore_wait(barrier, 3)

    table_msg = remote(table_ref.at[:, his_cols], tab.at[pl.ds(pl.multiple_of(core * rows_loc, rows_loc), rows_loc)], 0, partner)
    table_msg.start()

    def relay(m, q):
        return remote(looked.at[m, tok(rel(2), q)], r_relay.at[m, q], 1 + 2 * m + q, minus if m == 0 else plus)

    def direct(m, q):
        return remote(looked.at[m, tok(rel(1 if m == 0 else 3), q)], r_direct.at[m, q], 5 + 2 * m + q, plus if m == 0 else minus)

    def comb(m, q):
        return remote(s_comb.at[m, q], r_comb.at[m, q], 9 + 2 * m + q, minus if m == 0 else plus)

    def spread(q, way):
        here = xbuf.at[:, tok(chip, q), my_cols]
        return remote(here, here, 13 + 3 * q + way, (plus, minus, partner)[way])

    def far(q, m):
        here = xbuf.at[m, tok(rel(3 if m == 0 else 1), q), my_cols]
        return remote(here, here, 19 + 2 * q + m, plus if m == 0 else minus)

    def near_fwd(q, side):
        here = xbuf.at[:, tok(rel(3 if side == 0 else 1), q), my_cols]
        return remote(here, here, 23 + 2 * q + side, partner)

    def far_fwd(q, m):
        here = xbuf.at[m, tok(rel(2), q), my_cols]
        return remote(here, here, 27 + 2 * q + m, partner)

    def dn_msg(t):
        cols = pl.ds(pl.multiple_of(t * DN_TILE, DN_TILE), DN_TILE)
        return remote(dn2.at[0, :, :, cols], dnp.at[:, :, cols], 31 + t, partner)

    cp_tab.wait()
    table_msg.wait_recv()
    row_id = lax.broadcasted_iota(jnp.int32, (2 * rows_loc, seq_len), 0) + chip * (2 * rows_loc)
    for m in (1, 0):
        hot = jnp.where(row_id == ids_ref[m:m + 1, :], 1.0, 0.0).astype(BF16)
        looked[m] = lax.dot_general(hot, tab[...], (((0,), (0,)), ((), ())), preferred_element_type=F32).astype(BF16)
    for q in range(2):
        for m in range(2):
            relay(m, q).start()
    for q in range(2):
        for m in range(2):
            direct(m, q).start()
    cp_du.wait()

    def relay_step(q):
        for m in range(2):
            relay(m, q).wait_recv()
            s_comb[m, q] = looked[m, tok(rel(3 if m == 0 else 1), q)] + r_relay[m, q]
            comb(m, q).start()

    def sum_step(q):
        for m in range(2):
            direct(m, q).wait_recv()
            comb(m, q).wait_recv()
            xbuf[m, tok(chip, q), my_cols] = (looked[m, tok(chip, q)] + r_direct[m, q]) + r_comb[m, q]
        for way in range(3):
            spread(q, way).start()

    def dn_step(t, carry):
        @pl.when(t + 1 < 2 * tiles)
        def _():
            w_copy(t + 1).start()

        w_copy(t).wait()
        slot = lax.rem(t, 2)
        part = lax.dot_general(du_v[...].reshape(micro * seq_len, du_v.shape[2]), wbuf[slot], (((1,), (1,)), ((), ())),
                               preferred_element_type=F32).astype(BF16).reshape(micro, seq_len, DN_TILE)
        side = lax.div(t, tiles)
        col = (t - side * tiles) * DN_TILE
        dn2[side, :, :, pl.ds(pl.multiple_of(col, DN_TILE), DN_TILE)] = part

        @pl.when(t < tiles)
        def _():
            dn_msg(t).start()

        for q in range(2):
            @pl.when(t == RELAY_AT[q])
            def _():
                relay_step(q)
        for q in range(2):
            @pl.when(t == SUM_AT[q])
            def _():
                sum_step(q)
        return carry

    lax.fori_loop(0, 2 * tiles, dn_step, 0)

    def dn_wait(t, carry):
        dn_msg(t).wait_recv()
        return carry

    lax.fori_loop(0, tiles, dn_wait, 0)

    terms = ((2, 1), (1, 0), (2, 0), (3, 1), (1, 1), (3, 0), (0, 0), (0, 1))

    def s_copy(i):
        out = (plus_out, minus_out, keep_out, keep_out)[i // 2]
        return pltpu.make_async_copy(stage.at[i], out.at[i % 2 if i < 4 else i - 4], osem.at[i])

    def s_steps():
        for i, (j, m) in enumerate(terms):
            stage[i] = dn2[1, m, tok(rel(j))].astype(F32) + dnp[m, tok(rel(j))].astype(F32)
            s_copy(i).start()

    def near_step(q):
        spread(q, 0).wait_recv()
        far(q, 0).start()
        near_fwd(q, 0).start()
        spread(q, 1).wait_recv()
        far(q, 1).start()
        near_fwd(q, 1).start()

    near_step(0)
    s_steps()
    near_step(1)

    def n_copy(d, i):
        return pltpu.make_async_copy(n_v.at[:, tok(d)], n_out.at[:, tok(d)], osem.at[2 * chips + i])

    gain_f = gain_ref[...].astype(F32).reshape(1, model_dim)

    def norm_piece(j):
        d = rel(j)

        def body(i, carry):
            m, r = lax.div(i, ctok // 16), lax.rem(i, ctok // 16)
            rows = pl.ds(pl.multiple_of(d * ctok + r * 16, 16), 16)
            xf = xbuf[m, rows].astype(F32)
            inv = lax.rsqrt(jnp.mean(xf * xf, axis=-1, keepdims=True) + NORM_EPS)
            n_v[m, rows] = (xf * inv * gain_f).astype(BF16)
            return carry

        lax.fori_loop(0, micro * (ctok // 16), body, 0)
        n_copy(d, j).start()

    for q in range(2):
        spread(q, 2).wait_recv()
    cp_x = pltpu.make_async_copy(xbuf.at[:, tok(chip)], xchip_out, lsem.at[0])
    cp_x.start()
    norm_piece(0)
    for q in range(2):
        for m in range(2):
            far(q, m).wait_recv()
            far_fwd(q, m).start()
    for side, j in ((0, 3), (1, 1)):
        for q in range(2):
            near_fwd(q, side).wait_recv()
        norm_piece(j)
    for q in range(2):
        for m in range(2):
            far_fwd(q, m).wait_recv()
    norm_piece(2)

    for i in range(2 * chips):
        s_copy(i).wait()
    for j in range(chips):
        n_copy(rel(j), j).wait()
    cp_x.wait()
    table_msg.wait_send()
    for q in range(2):
        for m in range(2):
            relay(m, q).wait_send()
            direct(m, q).wait_send()
            comb(m, q).wait_send()
            far(q, m).wait_send()
            far_fwd(q, m).wait_send()
            near_fwd(q, m).wait_send()
        for way in range(3):
            spread(q, way).wait_send()

    def dn_drain(t, carry):
        dn_msg(t).wait_send()
        return carry

    lax.fori_loop(0, tiles, dn_drain, 0)


def gather_call(group, ids, gain2, table, w, du):
    micro, seq_len = ids.shape
    rows_loc, model_dim = table.shape
    cols_loc = w.shape[1]
    half = model_dim // 2
    chips = group // 2
    ctok = seq_len // chips
    tiles = half // DN_TILE
    hbm_spec = pl.BlockSpec(memory_space=pltpu.HBM)
    vmem_spec = pl.BlockSpec(memory_space=pltpu.VMEM)
    msg = pltpu.VMEM((2, 2, ctok // 2, half), BF16)
    total = micro * seq_len
    return pl.pallas_call(
        functools.partial(gather_kernel, group),
        out_shape=(jax.ShapeDtypeStruct((micro, seq_len, model_dim), BF16),
                   jax.ShapeDtypeStruct((micro, ctok, model_dim), BF16),
                   jax.ShapeDtypeStruct((2, ctok, half), F32),
                   jax.ShapeDtypeStruct((2, ctok, half), F32),
                   jax.ShapeDtypeStruct((4, ctok, half), F32)),
        in_specs=[vmem_spec, vmem_spec, hbm_spec, hbm_spec, hbm_spec],
        out_specs=(hbm_spec,) * 5,
        scratch_shapes=[
            pltpu.VMEM((2 * rows_loc, half), BF16),
            pltpu.VMEM((micro, seq_len, half), BF16),
            msg, msg, msg, msg,
            pltpu.VMEM((micro, seq_len, model_dim), BF16),
            pltpu.VMEM((micro, seq_len, model_dim), BF16),
            pltpu.VMEM((micro, seq_len, cols_loc), BF16),
            pltpu.VMEM((2, DN_TILE, cols_loc), BF16),
            pltpu.VMEM((2, micro, seq_len, half), BF16),
            pltpu.VMEM((micro, seq_len, half), BF16),
            pltpu.VMEM((2 * chips, ctok, half), F32),
            pltpu.SemaphoreType.DMA((2,)),
            pltpu.SemaphoreType.DMA((2,)),
            pltpu.SemaphoreType.DMA((3 * chips,)),
            pltpu.SemaphoreType.DMA((31 + tiles,)),
            pltpu.SemaphoreType.DMA((31 + tiles,)),
        ],
        compiler_params=pltpu.CompilerParams(collective_id=0, has_side_effects=True, vmem_limit_bytes=58 * 1024 * 1024),
        cost_estimate=pl.CostEstimate(flops=2 * total * cols_loc * model_dim, bytes_accessed=2 * cols_loc * model_dim, transcendentals=0),
        name="gather_dn",
    )(ids, gain2, table, w, du)


def weight_grad_kernel(n_ref, du_ref, out_ref, n_v, du_v, obuf, nsem, dsem, osem):
    _, model_dim = n_v.shape
    cols = du_v.shape[1]
    parts = cols // DW_COLS
    blocks = model_dim // DW_ROWS

    def at(i, n):
        return pl.ds(pl.multiple_of(i * n, n), n)

    def du_copy(j):
        return pltpu.make_async_copy(du_ref.at[:, at(j, DW_COLS)], du_v.at[:, at(j, DW_COLS)], dsem.at[j])

    def n_copy(i):
        return pltpu.make_async_copy(n_ref.at[:, at(i, DW_ROWS)], n_v.at[:, at(i, DW_ROWS)], nsem.at[i])

    def out_copy(s):
        i, j = lax.div(s, parts), lax.rem(s, parts)
        slot = lax.rem(s, DW_SLOTS)
        return pltpu.make_async_copy(obuf.at[slot], out_ref.at[at(i, DW_ROWS), at(j, DW_COLS)], osem.at[slot])

    n_copy(0).start()
    for j in range(parts):
        du_copy(j).start()
    for i in range(1, blocks):
        n_copy(i).start()

    def step(s, carry):
        i, j = lax.div(s, parts), lax.rem(s, parts)

        @pl.when(j == 0)
        def _():
            n_copy(i).wait()

        @pl.when(i == 0)
        def _():
            du_copy(j).wait()

        @pl.when(s >= DW_SLOTS)
        def _():
            out_copy(s - DW_SLOTS).wait()

        obuf[lax.rem(s, DW_SLOTS)] = lax.dot_general(n_v[:, at(i, DW_ROWS)], du_v[:, at(j, DW_COLS)], (((0,), (0,)), ((), ())),
                                                    preferred_element_type=F32)
        out_copy(s).start()
        return carry

    lax.fori_loop(0, blocks * parts, step, 0)

    def drain(s, carry):
        out_copy(s).wait()
        return carry

    lax.fori_loop(blocks * parts - DW_SLOTS, blocks * parts, drain, 0)


def weight_grad_call(n2, du2):
    total, model_dim = n2.shape
    cols = du2.shape[1]
    any_spec = pl.BlockSpec(memory_space=pl.ANY)
    return pl.pallas_call(
        weight_grad_kernel,
        out_shape=jax.ShapeDtypeStruct((model_dim, cols), F32),
        in_specs=[any_spec, any_spec],
        out_specs=any_spec,
        scratch_shapes=[
            pltpu.VMEM((total, model_dim), BF16),
            pltpu.VMEM((total, cols), BF16),
            pltpu.VMEM((DW_SLOTS, DW_ROWS, DW_COLS), F32),
            pltpu.SemaphoreType.DMA((model_dim // DW_ROWS,)),
            pltpu.SemaphoreType.DMA((cols // DW_COLS,)),
            pltpu.SemaphoreType.DMA((DW_SLOTS,)),
        ],
        compiler_params=pltpu.CompilerParams(vmem_limit_bytes=63 * 1024 * 1024),
        cost_estimate=pl.CostEstimate(flops=2 * total * cols * model_dim, bytes_accessed=4 * cols * model_dim, transcendentals=0),
        name="weight_grad",
    )(n2, du2)


def finish_kernel(group, ids_ref, gain_ref, rp_ref, rm_ref, keep_ref, xchip_ref, dres_ref, n_ref, w_ref,
                  u_out, dx_out, dg_out,
                  rp, rm, keep, xc, dres, n_v, wbuf, ubuf, s_comb, r_comb, dn_v, dot_s, dot_r, dxbuf, dg_v, dg_r, dg_half,
                  lsem, wsem, usem, osem, snd, rcv):
    dev = lax.axis_index('tp')
    chips = group // 2
    chip = lax.div(dev, 2)
    core = lax.rem(dev, 2)
    plus = lax.rem(dev + 2, group)
    minus = lax.rem(dev + group - 2, group)
    opposite = lax.rem(dev + group // 2, group)
    partner = dev + 1 - 2 * core
    micro, seq_len = ids_ref.shape
    model_dim = gain_ref.shape[0]
    half = model_dim // 2
    ctok = seq_len // chips
    qrows = ctok // 2
    u_cols = wbuf.shape[2]
    steps = w_ref.shape[1] // u_cols
    total = micro * seq_len
    my_cols = pl.ds(pl.multiple_of(core * half, 128), half)
    his_cols = pl.ds(pl.multiple_of((1 - core) * half, 128), half)

    def rel(j):
        return lax.rem(chip + j, chips)

    def tok(d, q=None):
        if q is None:
            return pl.ds(pl.multiple_of(d * ctok, ctok), ctok)
        return pl.ds(pl.multiple_of(d * ctok + q * qrows, qrows), qrows)

    def remote(src, dst, slot, target):
        return pltpu.make_async_remote_copy(src_ref=src, dst_ref=dst, send_sem=snd.at[slot], recv_sem=rcv.at[slot],
                                            device_id={'tp': target}, device_id_type=MESH)

    def local(src, dst, i):
        return pltpu.make_async_copy(src, dst, lsem.at[i])

    own_rows = pl.ds(pl.multiple_of(core * qrows, qrows), qrows)
    loads = [local(rp_ref, rp, 0), local(rm_ref, rm, 1), local(keep_ref, keep, 2), local(xchip_ref, xc, 3),
             local(n_ref, n_v, 4), local(dres_ref.at[:, :, my_cols], dres.at[:, own_rows], 5)]
    for cp in loads[:4]:
        cp.start()

    def w_copy(t):
        slot = lax.rem(t, 2)
        return pltpu.make_async_copy(w_ref.at[:, pl.ds(pl.multiple_of(t * u_cols, u_cols), u_cols)], wbuf.at[slot], wsem.at[slot])

    def u_copy(t):
        slot = lax.rem(t, 2)
        return pltpu.make_async_copy(ubuf.at[slot], u_out.at[:, :, pl.ds(pl.multiple_of(t * u_cols, u_cols), u_cols)], usem.at[slot])

    loads[4].start()
    loads[5].start()
    w_copy(0).start()

    barrier = pltpu.get_barrier_semaphore()
    for target in (plus, minus, partner, opposite):
        pl.semaphore_signal(barrier, inc=1, device_id={'tp': target}, device_id_type=MESH)
    pl.semaphore_wait(barrier, 4)

    dres_msg = remote(dres_ref.at[:, :, his_cols], dres.at[:, own_rows], 0, partner)
    dres_msg.start()

    def comb(m, q):
        return remote(s_comb.at[m, q], r_comb.at[m, q], 1 + 2 * m + q, minus if m == 0 else plus)

    def dot_msg(q):
        return remote(dot_s.at[q], dot_r.at[q], 5 + q, partner)

    def spread(q, way):
        here = dxbuf.at[:, tok(chip, q), my_cols]
        return remote(here, here, 7 + 3 * q + way, (plus, minus, partner)[way])

    def far(q, m):
        here = dxbuf.at[m, tok(rel(3 if m == 0 else 1), q), my_cols]
        return remote(here, here, 13 + 2 * q + m, plus if m == 0 else minus)

    def near_fwd(q, side):
        here = dxbuf.at[:, tok(rel(3 if side == 0 else 1), q), my_cols]
        return remote(here, here, 17 + 2 * q + side, partner)

    def far_fwd(q, m):
        here = dxbuf.at[m, tok(rel(2), q), my_cols]
        return remote(here, here, 21 + 2 * q + m, partner)

    def dg_msg(way):
        return remote(dg_v, dg_r.at[way], 25 + way, (plus, minus, opposite)[way])

    dg_fin = remote(dg_half.at[0], dg_half.at[1], 28, partner)

    for cp in loads[:4]:
        cp.wait()
    for q in range(2):
        rows = slice(q * qrows, (q + 1) * qrows)
        s_comb[1, q] = keep[0, rows] + rp[0, rows]
        comb(1, q).start()
        s_comb[0, q] = keep[1, rows] + rm[0, rows]
        comb(0, q).start()
    for cp in loads[4:]:
        cp.wait()
    dres_msg.wait_recv()
    gain_half = gain_ref[my_cols].astype(F32).reshape(1, half)

    def hat_of(m, rows):
        xf = xc[m, rows].astype(F32)
        inv = lax.rsqrt(jnp.mean(xf * xf, axis=-1, keepdims=True) + NORM_EPS)
        return xc[m, rows, my_cols].astype(F32) * inv, inv

    def dn_finish(q):
        rows = slice(q * qrows, (q + 1) * qrows)
        part = jnp.zeros((1, half), F32)
        for m in range(2):
            comb(m, q).wait_recv()
            direct = rp[1, rows] if m == 0 else rm[1, rows]
            dn = keep[2 + m, rows] + direct + r_comb[m, q]
            dn_v[m, rows] = dn
            hat, _ = hat_of(m, rows)
            prod = dn * hat
            part = part + jnp.sum(prod, axis=0, keepdims=True)
            dots = jnp.sum(prod * gain_half, axis=-1, keepdims=True)
            dot_s[q, m] = jnp.broadcast_to(dots, (qrows, 128))
        dot_msg(q).start()
        if q == 0:
            dg_v[...] = part
        else:
            dg_v[...] += part
            for way in range(3):
                dg_msg(way).start()

    def dx_finish(q):
        rows = slice(q * qrows, (q + 1) * qrows)
        dot_msg(q).wait_recv()
        for m in range(2):
            hat, inv = hat_of(m, rows)
            centre = (dot_s[q, m, :, :1] + dot_r[q, m, :, :1]) * (1.0 / model_dim)
            dx = dres[m, rows].astype(F32) + inv * (gain_half * dn_v[m, rows] - hat * centre)
            dxbuf[m, tok(chip, q), my_cols] = dx.astype(BF16)
        for way in range(3):
            spread(q, way).start()

    def near_step(q):
        spread(q, 0).wait_recv()
        far(q, 0).start()
        near_fwd(q, 0).start()
        spread(q, 1).wait_recv()
        far(q, 1).start()
        near_fwd(q, 1).start()

    def dg_step():
        for way in range(3):
            dg_msg(way).wait_recv()
        dg_half[0] = dg_v[...] + dg_r[0] + dg_r[1] + dg_r[2]
        dg_fin.start()

    hooks = ((U_HOOKS[0], lambda: dn_finish(0)), (U_HOOKS[1], lambda: dx_finish(0)), (U_HOOKS[2], lambda: dn_finish(1)),
             (U_HOOKS[3], lambda: dx_finish(1)), (U_HOOKS[4], lambda: near_step(0)), (U_HOOKS[5], dg_step))

    def u_step(t, carry):
        @pl.when(t + 1 < steps)
        def _():
            w_copy(t + 1).start()

        w_copy(t).wait()

        @pl.when(t >= 2)
        def _():
            u_copy(t - 2).wait()

        slot = lax.rem(t, 2)
        ubuf[slot] = jnp.dot(n_v[...].reshape(total, model_dim), wbuf[slot], preferred_element_type=F32).astype(BF16).reshape(micro, seq_len, u_cols)
        u_copy(t).start()
        for at, hook in hooks:
            pl.when(t == at)(hook)
        return carry

    lax.fori_loop(0, steps, u_step, 0)
    near_step(1)
    for q in range(2):
        for m in range(2):
            far(q, m).wait_recv()
            far_fwd(q, m).start()
    dg_fin.wait_recv()
    dg_copies = [pltpu.make_async_copy(dg_half.at[0], dg_out.at[:, my_cols], osem.at[0]),
                 pltpu.make_async_copy(dg_half.at[1], dg_out.at[:, his_cols], osem.at[1])]
    for cp in dg_copies:
        cp.start()
    for q in range(2):
        spread(q, 2).wait_recv()
        for side in range(2):
            near_fwd(q, side).wait_recv()
    near_copies = [pltpu.make_async_copy(dxbuf.at[:, tok(rel(j))], dx_out.at[:, tok(rel(j))], osem.at[2 + j]) for j in range(chips)]
    for j in (0, 1, 3):
        near_copies[j].start()
    for q in range(2):
        for side in range(2):
            far_fwd(q, side).wait_recv()
    near_copies[2].start()

    for cp in near_copies:
        cp.wait()
    for cp in dg_copies:
        cp.wait()
    u_copy(steps - 2).wait()
    u_copy(steps - 1).wait()
    dres_msg.wait_send()
    dg_fin.wait_send()
    for way in range(3):
        dg_msg(way).wait_send()
    for q in range(2):
        dot_msg(q).wait_send()
        for m in range(2):
            comb(m, q).wait_send()
            far(q, m).wait_send()
            far_fwd(q, m).wait_send()
            near_fwd(q, m).wait_send()
        for way in range(3):
            spread(q, way).wait_send()


def finish_call(group, ids, gain2, rp, rm, keep, xchip, dres, n3, w):
    micro, seq_len = ids.shape
    model_dim, cols_loc = w.shape
    half = model_dim // 2
    chips = group // 2
    ctok = seq_len // chips
    qrows = ctok // 2
    total = micro * seq_len
    hbm_spec = pl.BlockSpec(memory_space=pltpu.HBM)
    any_spec = pl.BlockSpec(memory_space=pl.ANY)
    vmem_spec = pl.BlockSpec(memory_space=pltpu.VMEM)
    return pl.pallas_call(
        functools.partial(finish_kernel, group),
        out_shape=(jax.ShapeDtypeStruct((micro, seq_len, cols_loc), BF16),
                   jax.ShapeDtypeStruct((micro, seq_len, model_dim), BF16),
                   jax.ShapeDtypeStruct((1, model_dim), F32)),
        in_specs=[vmem_spec, vmem_spec] + [hbm_spec] * 7,
        out_specs=(any_spec,) * 3,
        scratch_shapes=[
            pltpu.VMEM((2, ctok, half), F32),
            pltpu.VMEM((2, ctok, half), F32),
            pltpu.VMEM((4, ctok, half), F32),
            pltpu.VMEM((micro, ctok, model_dim), BF16),
            pltpu.VMEM((micro, ctok, half), BF16),
            pltpu.VMEM((micro, seq_len, model_dim), BF16),
            pltpu.VMEM((2, model_dim, U_COLS), BF16),
            pltpu.VMEM((2, micro, seq_len, U_COLS), BF16),
            pltpu.VMEM((2, 2, qrows, half), F32),
            pltpu.VMEM((2, 2, qrows, half), F32),
            pltpu.VMEM((micro, ctok, half), F32),
            pltpu.VMEM((2, micro, qrows, 128), F32),
            pltpu.VMEM((2, micro, qrows, 128), F32),
            pltpu.VMEM((micro, seq_len, model_dim), BF16),
            pltpu.VMEM((1, half), F32),
            pltpu.VMEM((3, 1, half), F32),
            pltpu.VMEM((2, 1, half), F32),
            pltpu.SemaphoreType.DMA((6,)),
            pltpu.SemaphoreType.DMA((2,)),
            pltpu.SemaphoreType.DMA((2,)),
            pltpu.SemaphoreType.DMA((2 + chips,)),
            pltpu.SemaphoreType.DMA((29,)),
            pltpu.SemaphoreType.DMA((29,)),
        ],
        compiler_params=pltpu.CompilerParams(collective_id=1, has_side_effects=True, vmem_limit_bytes=30 * 1024 * 1024),
        cost_estimate=pl.CostEstimate(flops=2 * total * cols_loc * model_dim, bytes_accessed=2 * cols_loc * model_dim, transcendentals=0),
        name="finish_u",
    )(ids, gain2, *[pltpu.with_memory_space_constraint(v, pltpu.HBM) for v in (rp, rm, keep, xchip, dres, n3, w)])


def epilogue_kernel(ids_ref, u_ref, dx_ref, dg_ref, xchip_ref, u_out, de_out, dg_out, x_out, u_v, dx_v, de_v, x_v, usem, xsem, osem):
    dev = lax.axis_index('tp')
    own_tok = x_v.shape[1]
    own_rows = pl.ds(pl.multiple_of(lax.rem(dev, 2) * own_tok, own_tok), own_tok)
    own_in = pltpu.make_async_copy(xchip_ref.at[:, own_rows], x_v, osem.at[0])
    own_out = pltpu.make_async_copy(x_v, x_out, osem.at[1])
    micro, seq_len = ids_ref.shape
    rows_loc, model_dim = de_v.shape
    steps = model_dim // DE_COLS
    ucols = u_v.shape[2] // U_PARTS

    def cols(i, n):
        return pl.ds(i * n, n)

    x_loads = [pltpu.make_async_copy(dx_ref.at[:, :, cols(i, DE_COLS)], dx_v.at[:, :, cols(i, DE_COLS)], xsem.at[i]) for i in range(steps)]
    u_loads = [pltpu.make_async_copy(u_ref.at[:, :, cols(i, ucols)], u_v.at[:, :, cols(i, ucols)], usem.at[i]) for i in range(U_PARTS)]
    x_loads[0].start()
    x_loads[1].start()
    for cp in u_loads:
        cp.start()
    for cp in x_loads[2:]:
        cp.start()
    own_in.start()
    dg_out[...] = dg_ref[0]
    row_id = lax.broadcasted_iota(jnp.int32, (rows_loc, seq_len), 0) + dev * rows_loc
    hot = jnp.concatenate([jnp.where(row_id == ids_ref[m:m + 1, :], 1.0, 0.0).astype(BF16) for m in range(micro)], axis=1)
    u_stores = [pltpu.make_async_copy(u_v.at[:, :, cols(i, ucols)], u_out.at[:, :, cols(i, ucols)], usem.at[U_PARTS + i]) for i in range(U_PARTS)]
    de_stores = [pltpu.make_async_copy(de_v.at[:, cols(i, DE_COLS)], de_out.at[:, cols(i, DE_COLS)], xsem.at[steps + i]) for i in range(steps)]
    for i in range(steps):
        x_loads[i].wait()
        de_v[:, cols(i, DE_COLS)] = jnp.dot(hot, dx_v[:, :, cols(i, DE_COLS)].reshape(micro * seq_len, DE_COLS), preferred_element_type=F32)
        de_stores[i].start()
        if i < U_PARTS:
            u_loads[i].wait()
            u_stores[i].start()
    own_in.wait()
    own_out.start()
    for cp in u_stores + de_stores + [own_out]:
        cp.wait()


def epilogue_call(rows_loc, ids, u, dx, dg, xchip):
    micro, seq_len, _ = u.shape
    model_dim = dx.shape[2]
    steps = model_dim // DE_COLS
    any_spec = pl.BlockSpec(memory_space=pl.ANY)
    vmem_spec = pl.BlockSpec(memory_space=pltpu.VMEM)
    return pl.pallas_call(
        epilogue_kernel,
        out_shape=(jax.ShapeDtypeStruct(u.shape, BF16), jax.ShapeDtypeStruct((rows_loc, model_dim), F32),
                   jax.ShapeDtypeStruct((model_dim,), F32),
                   jax.ShapeDtypeStruct((micro, xchip.shape[1] // 2, model_dim), BF16)),
        in_specs=[vmem_spec, any_spec, any_spec, vmem_spec, any_spec],
        out_specs=(any_spec, any_spec, vmem_spec, any_spec),
        scratch_shapes=[
            pltpu.VMEM(u.shape, BF16),
            pltpu.VMEM(dx.shape, BF16),
            pltpu.VMEM((rows_loc, model_dim), F32),
            pltpu.VMEM((micro, xchip.shape[1] // 2, model_dim), BF16),
            pltpu.SemaphoreType.DMA((2 * U_PARTS,)),
            pltpu.SemaphoreType.DMA((2 * steps,)),
            pltpu.SemaphoreType.DMA((2,)),
        ],
        compiler_params=pltpu.CompilerParams(vmem_limit_bytes=22 * 1024 * 1024),
        cost_estimate=pl.CostEstimate(flops=2 * micro * seq_len * rows_loc * model_dim, bytes_accessed=4 * rows_loc * model_dim, transcendentals=0),
        name="epilogue",
    )(ids, u, dx, dg, xchip)


def solution(mesh):
    group = mesh.shape['tp']
    plus = [(r, (r + 2) % group) for r in range(group)]
    minus = [(r, (r - 2) % group) for r in range(group)]

    def local_step(token_ids, table_loc, gain_vec, w_loc, du_loc, dres_loc):
        micro, seq_len = token_ids.shape
        model_dim, cols_loc = w_loc.shape
        total = micro * seq_len
        gain2 = gain_vec
        normed, x_chip, msg_plus, msg_minus, keep = gather_call(group, token_ids, gain2, table_loc, w_loc, du_loc)
        got_plus = lax.ppermute(msg_plus, 'tp', plus)
        got_minus = lax.ppermute(msg_minus, 'tp', minus)
        grad_w = weight_grad_call(normed.reshape(total, model_dim), du_loc.reshape(total, cols_loc))
        u_tmp, dx_all, dg = finish_call(group, token_ids, gain2, got_plus, got_minus, keep, x_chip, dres_loc, normed, w_loc)
        u, grad_table, grad_gain, x_own = epilogue_call(table_loc.shape[0], token_ids, u_tmp, dx_all, dg, x_chip)
        return u, x_own, grad_table, grad_w, grad_gain

    return jax.shard_map(local_step, mesh=mesh,
                         in_specs=(P('dp', None), P('tp', None), P(None), P(None, 'tp'), P('dp', None, 'tp'), P('dp', 'tp', None)),
                         out_specs=(P('dp', None, 'tp'), P('dp', 'tp', None), P(('dp', 'tp'), None), P(None, ('dp', 'tp')), P('dp')),
                         check_vma=False)
```

```python
import functools

import jax
import jax.numpy as jnp
from jax import lax
from jax.experimental import pallas as pl
from jax.experimental.pallas import tpu as pltpu
from jax.sharding import PartitionSpec as P

NORM_EPS = 1e-6
MESH = pl.DeviceIdType.MESH
F32 = jnp.float32
BF16 = jnp.bfloat16
DN_TILE = 256
RELAY_AT = (2, 4)
SUM_AT = (9, 10)
DW_ROWS = 256
DW_COLS = 2304
U_COLS = 256
U_HOOKS = (3, 4, 6, 7, 9, 11, 13, 15)
DE_COLS = 512
U_PARTS = 4


def gather_kernel(group, ids_ref, gain_ref, table_ref, w_ref, du_ref,
                  n_out, xchip_out, plus_out, minus_out, keep_out,
                  tab, hot, looked, r_relay, r_direct, r_comb, s_comb, xbuf, n_v, du_v, wbuf, dn2, dnp, stage,
                  lsem, wsem, osem, snd, rcv):
    dev = lax.axis_index('tp')
    chips = group // 2
    chip = lax.div(dev, 2)
    core = lax.rem(dev, 2)
    plus = lax.rem(dev + 2, group)
    minus = lax.rem(dev + group - 2, group)
    partner = dev + 1 - 2 * core
    micro, seq_len = ids_ref.shape
    rows_loc, model_dim = table_ref.shape
    half = model_dim // 2
    ctok = seq_len // chips
    qrows = ctok // 2
    tiles = half // DN_TILE
    my_cols = pl.ds(pl.multiple_of(core * half, 128), half)
    his_cols = pl.ds(pl.multiple_of((1 - core) * half, 128), half)

    def rel(j):
        return lax.rem(chip + j, chips)

    def tok(d, q=None):
        if q is None:
            return pl.ds(pl.multiple_of(d * ctok, ctok), ctok)
        return pl.ds(pl.multiple_of(d * ctok + q * qrows, qrows), qrows)

    def remote(src, dst, slot, target):
        return pltpu.make_async_remote_copy(src_ref=src, dst_ref=dst, send_sem=snd.at[slot], recv_sem=rcv.at[slot],
                                            device_id={'tp': target}, device_id_type=MESH)

    cp_du = pltpu.make_async_copy(du_ref, du_v, lsem.at[0])
    cp_tab = pltpu.make_async_copy(table_ref.at[:, my_cols],
                                   tab.at[pl.ds(pl.multiple_of(core * rows_loc, rows_loc), rows_loc)], lsem.at[1])

    def w_copy(t):
        ft = jnp.where(t < tiles, (1 - core) * tiles + t, core * tiles + t - tiles)
        slot = lax.rem(t, 2)
        return pltpu.make_async_copy(w_ref.at[pl.ds(pl.multiple_of(ft * DN_TILE, DN_TILE), DN_TILE), :], wbuf.at[slot],
                                     wsem.at[slot])

    cp_tab.start()
    cp_du.start()
    w_copy(0).start()

    barrier = pltpu.get_barrier_semaphore()
    for target in (plus, minus, partner):
        pl.semaphore_signal(barrier, inc=1, device_id={'tp': target}, device_id_type=MESH)
    pl.semaphore_wait(barrier, 3)

    table_msg = remote(table_ref.at[:, his_cols], tab.at[pl.ds(pl.multiple_of(core * rows_loc, rows_loc), rows_loc)], 0, partner)
    table_msg.start()

    def relay(m, q):
        return remote(looked.at[m, tok(rel(2), q)], r_relay.at[m, q], 1 + 2 * m + q, minus if m == 0 else plus)

    def direct(m, q):
        return remote(looked.at[m, tok(rel(1 if m == 0 else 3), q)], r_direct.at[m, q], 5 + 2 * m + q, plus if m == 0 else minus)

    def comb(m, q):
        return remote(s_comb.at[m, q], r_comb.at[m, q], 9 + 2 * m + q, minus if m == 0 else plus)

    def spread(q, way):
        here = xbuf.at[:, tok(chip, q), my_cols]
        return remote(here, here, 13 + 3 * q + way, (plus, minus, partner)[way])

    def far(q, m):
        here = xbuf.at[m, tok(rel(3 if m == 0 else 1), q), my_cols]
        return remote(here, here, 19 + 2 * q + m, plus if m == 0 else minus)

    def near_fwd(q, side):
        here = xbuf.at[:, tok(rel(3 if side == 0 else 1), q), my_cols]
        return remote(here, here, 23 + 2 * q + side, partner)

    def far_fwd(q, m):
        here = xbuf.at[m, tok(rel(2), q), my_cols]
        return remote(here, here, 27 + 2 * q + m, partner)

    def dn_msg(t):
        cols = pl.ds(pl.multiple_of(t * DN_TILE, DN_TILE), DN_TILE)
        return remote(dn2.at[0, :, :, cols], dnp.at[:, :, cols], 31 + t, partner)

    row_id = lax.broadcasted_iota(jnp.int32, (2 * rows_loc, seq_len), 0) + chip * (2 * rows_loc)
    for m in range(micro):
        hot[m] = jnp.where(row_id == ids_ref[m:m + 1, :], 1.0, 0.0).astype(BF16).T
    cp_tab.wait()
    table_msg.wait_recv()
    for m in range(micro):
        looked[m] = jnp.dot(hot[m], tab[...], preferred_element_type=F32).astype(BF16)
    for q in range(2):
        for m in range(2):
            relay(m, q).start()
    for q in range(2):
        for m in range(2):
            direct(m, q).start()
    cp_du.wait()

    def relay_step(q):
        for m in range(2):
            relay(m, q).wait_recv()
            s_comb[m, q] = looked[m, tok(rel(3 if m == 0 else 1), q)] + r_relay[m, q]
            comb(m, q).start()

    def sum_step(q):
        for m in range(2):
            direct(m, q).wait_recv()
            comb(m, q).wait_recv()
            xbuf[m, tok(chip, q), my_cols] = (looked[m, tok(chip, q)] + r_direct[m, q]) + r_comb[m, q]
        for way in range(3):
            spread(q, way).start()

    def dn_step(t, carry):
        @pl.when(t + 1 < 2 * tiles)
        def _():
            w_copy(t + 1).start()

        w_copy(t).wait()
        slot = lax.rem(t, 2)
        part = lax.dot_general(du_v[...].reshape(micro * seq_len, du_v.shape[2]), wbuf[slot], (((1,), (1,)), ((), ())),
                               preferred_element_type=F32).astype(BF16).reshape(micro, seq_len, DN_TILE)
        side = lax.div(t, tiles)
        col = (t - side * tiles) * DN_TILE
        dn2[side, :, :, pl.ds(pl.multiple_of(col, DN_TILE), DN_TILE)] = part

        @pl.when(t < tiles)
        def _():
            dn_msg(t).start()

        for q in range(2):
            @pl.when(t == RELAY_AT[q])
            def _():
                relay_step(q)
        for q in range(2):
            @pl.when(t == SUM_AT[q])
            def _():
                sum_step(q)
        return carry

    lax.fori_loop(0, 2 * tiles, dn_step, 0)


    terms = ((2, 1), (1, 0), (2, 0), (3, 1), (1, 1), (3, 0), (0, 0), (0, 1))

    def s_copy(i):
        out = (plus_out, minus_out, keep_out, keep_out)[i // 2]
        return pltpu.make_async_copy(stage.at[i], out.at[i % 2 if i < 4 else i - 4], osem.at[i])

    def s_steps():
        for i, (j, m) in enumerate(terms):
            stage[i] = dn2[1, m, tok(rel(j))].astype(F32) + dnp[m, tok(rel(j))].astype(F32)
            s_copy(i).start()

    def near_step(q):
        spread(q, 0).wait_recv()
        far(q, 0).start()
        near_fwd(q, 0).start()
        spread(q, 1).wait_recv()
        far(q, 1).start()
        near_fwd(q, 1).start()

    def dn_wait(t, carry):
        dn_msg(t).wait_recv()
        return carry

    near_step(0)
    lax.fori_loop(0, tiles, dn_wait, 0)
    s_steps()
    near_step(1)

    def n_copy(d, i):
        return pltpu.make_async_copy(n_v.at[:, tok(d)], n_out.at[:, tok(d)], osem.at[2 * chips + i])

    gain_f = gain_ref[...].astype(F32).reshape(1, model_dim)

    def norm_piece(j):
        d = rel(j)

        def body(i, carry):
            m, r = lax.div(i, ctok // 16), lax.rem(i, ctok // 16)
            rows = pl.ds(pl.multiple_of(d * ctok + r * 16, 16), 16)
            xf = xbuf[m, rows].astype(F32)
            inv = lax.rsqrt(jnp.mean(xf * xf, axis=-1, keepdims=True) + NORM_EPS)
            n_v[m, rows] = (xf * inv * gain_f).astype(BF16)
            return carry

        lax.fori_loop(0, micro * (ctok // 16), body, 0)
        n_copy(d, j).start()

    for q in range(2):
        spread(q, 2).wait_recv()
    cp_x = pltpu.make_async_copy(xbuf.at[:, tok(chip)], xchip_out, lsem.at[0])
    cp_x.start()
    norm_piece(0)
    for q in range(2):
        for m in range(2):
            far(q, m).wait_recv()
            far_fwd(q, m).start()
    for side, j in ((0, 3), (1, 1)):
        for q in range(2):
            near_fwd(q, side).wait_recv()
        norm_piece(j)
    for q in range(2):
        for m in range(2):
            far_fwd(q, m).wait_recv()
    norm_piece(2)

    for i in range(2 * chips):
        s_copy(i).wait()
    for j in range(chips):
        n_copy(rel(j), j).wait()
    cp_x.wait()
    table_msg.wait_send()
    for q in range(2):
        for m in range(2):
            relay(m, q).wait_send()
            direct(m, q).wait_send()
            comb(m, q).wait_send()
            far(q, m).wait_send()
            far_fwd(q, m).wait_send()
            near_fwd(q, m).wait_send()
        for way in range(3):
            spread(q, way).wait_send()

    def dn_drain(t, carry):
        dn_msg(t).wait_send()
        return carry

    lax.fori_loop(0, tiles, dn_drain, 0)


def gather_call(group, ids, gain2, table, w, du):
    micro, seq_len = ids.shape
    rows_loc, model_dim = table.shape
    cols_loc = w.shape[1]
    half = model_dim // 2
    chips = group // 2
    ctok = seq_len // chips
    tiles = half // DN_TILE
    hbm_spec = pl.BlockSpec(memory_space=pltpu.HBM)
    vmem_spec = pl.BlockSpec(memory_space=pltpu.VMEM)
    msg = pltpu.VMEM((2, 2, ctok // 2, half), BF16)
    total = micro * seq_len
    return pl.pallas_call(
        functools.partial(gather_kernel, group),
        out_shape=(jax.ShapeDtypeStruct((micro, seq_len, model_dim), BF16),
                   jax.ShapeDtypeStruct((micro, ctok, model_dim), BF16),
                   jax.ShapeDtypeStruct((2, ctok, half), F32),
                   jax.ShapeDtypeStruct((2, ctok, half), F32),
                   jax.ShapeDtypeStruct((4, ctok, half), F32)),
        in_specs=[vmem_spec, vmem_spec, hbm_spec, hbm_spec, hbm_spec],
        out_specs=(hbm_spec,) * 5,
        scratch_shapes=[
            pltpu.VMEM((2 * rows_loc, half), BF16),
            pltpu.VMEM((micro, seq_len, 2 * rows_loc), BF16),
            pltpu.VMEM((micro, seq_len, half), BF16),
            msg, msg, msg, msg,
            pltpu.VMEM((micro, seq_len, model_dim), BF16),
            pltpu.VMEM((micro, seq_len, model_dim), BF16),
            pltpu.VMEM((micro, seq_len, cols_loc), BF16),
            pltpu.VMEM((2, DN_TILE, cols_loc), BF16),
            pltpu.VMEM((2, micro, seq_len, half), BF16),
            pltpu.VMEM((micro, seq_len, half), BF16),
            pltpu.VMEM((2 * chips, ctok, half), F32),
            pltpu.SemaphoreType.DMA((2,)),
            pltpu.SemaphoreType.DMA((2,)),
            pltpu.SemaphoreType.DMA((3 * chips,)),
            pltpu.SemaphoreType.DMA((31 + tiles,)),
            pltpu.SemaphoreType.DMA((31 + tiles,)),
        ],
        compiler_params=pltpu.CompilerParams(collective_id=0, has_side_effects=True, vmem_limit_bytes=58 * 1024 * 1024),
        cost_estimate=pl.CostEstimate(flops=2 * total * cols_loc * model_dim, bytes_accessed=2 * cols_loc * model_dim, transcendentals=0),
        name="gather_dn",
    )(ids, gain2, table, w, du)


def weight_grad_kernel(n_ref, du_ref, out_ref, n_v, du_v, even, odd, obuf, nsem, dsem, osem):
    _, model_dim = n_v.shape
    cols = du_v.shape[1]
    parts = cols // DW_COLS
    blocks = model_dim // DW_ROWS

    def at(i, n):
        return pl.ds(pl.multiple_of(i * n, n), n)

    def du_copy(j):
        return pltpu.make_async_copy(du_ref.at[:, at(j, DW_COLS)], du_v.at[:, at(j, DW_COLS)], dsem.at[j])

    def n_copy(i):
        return pltpu.make_async_copy(n_ref.at[:, at(i, DW_ROWS)], n_v.at[:, at(i, DW_ROWS)], nsem.at[i])

    def out_copy(s, slot):
        i, j = lax.div(s, parts), lax.rem(s, parts)
        return pltpu.make_async_copy(obuf.at[slot], out_ref.at[at(i, DW_ROWS), at(j, DW_COLS)], osem.at[slot])

    n_copy(0).start()
    for j in range(parts):
        du_copy(j).start()
    for i in range(1, blocks):
        n_copy(i).start()
    n_copy(0).wait()
    even[...] = n_v[:, at(0, DW_ROWS)].T

    def pair(p, carry):
        for e in range(2):
            i = 2 * p + e
            here, there = (even, odd) if e == 0 else (odd, even)
            nxt = jnp.minimum(i + 1, blocks - 1)

            @pl.when(i + 1 < blocks)
            def _():
                n_copy(i + 1).wait()

            for j in range(parts):
                slot = e * parts + j

                @pl.when(i == 0)
                def _():
                    du_copy(j).wait()

                @pl.when(p > 0)
                def _():
                    out_copy((i - 2) * parts + j, slot).wait()
            there[...] = n_v[:, at(nxt, DW_ROWS)].T
            for j in range(parts):
                slot = e * parts + j
                obuf[slot] = jnp.dot(here[...], du_v[:, j * DW_COLS:(j + 1) * DW_COLS], preferred_element_type=F32)
                out_copy(i * parts + j, slot).start()
        return carry

    lax.fori_loop(0, blocks // 2, pair, 0)
    for e in range(2):
        for j in range(parts):
            out_copy((blocks - 2 + e) * parts + j, e * parts + j).wait()


def weight_grad_call(n2, du2):
    total, model_dim = n2.shape
    cols = du2.shape[1]
    any_spec = pl.BlockSpec(memory_space=pl.ANY)
    return pl.pallas_call(
        weight_grad_kernel,
        out_shape=jax.ShapeDtypeStruct((model_dim, cols), F32),
        in_specs=[any_spec, any_spec],
        out_specs=any_spec,
        scratch_shapes=[
            pltpu.VMEM((total, model_dim), BF16),
            pltpu.VMEM((total, cols), BF16),
            pltpu.VMEM((DW_ROWS, total), BF16),
            pltpu.VMEM((DW_ROWS, total), BF16),
            pltpu.VMEM((2 * cols // DW_COLS, DW_ROWS, DW_COLS), F32),
            pltpu.SemaphoreType.DMA((model_dim // DW_ROWS,)),
            pltpu.SemaphoreType.DMA((cols // DW_COLS,)),
            pltpu.SemaphoreType.DMA((2 * cols // DW_COLS,)),
        ],
        compiler_params=pltpu.CompilerParams(vmem_limit_bytes=67043328),
        cost_estimate=pl.CostEstimate(flops=2 * total * cols * model_dim, bytes_accessed=4 * cols * model_dim, transcendentals=0),
        name="weight_grad",
    )(n2, du2)


def finish_kernel(group, gain_hbm, rp_ref, rm_ref, keep_ref, xchip_ref, dres_ref, n_ref, w_ref,
                  u_out, dx_out, dg_out,
                  gain_ref, rp, rm, keep, xc, dres, n_v, wbuf, ubuf, s_comb, r_comb, dn_v, dot_s, dot_r, dxbuf, dg_v, dg_r, dg_half,
                  lsem, wsem, usem, osem, snd, rcv):
    dev = lax.axis_index('tp')
    chips = group // 2
    chip = lax.div(dev, 2)
    core = lax.rem(dev, 2)
    plus = lax.rem(dev + 2, group)
    minus = lax.rem(dev + group - 2, group)
    opposite = lax.rem(dev + group // 2, group)
    partner = dev + 1 - 2 * core
    micro, seq_len, model_dim = n_ref.shape
    half = model_dim // 2
    ctok = seq_len // chips
    qrows = ctok // 2
    u_cols = wbuf.shape[2]
    steps = w_ref.shape[1] // u_cols
    total = micro * seq_len
    my_cols = pl.ds(pl.multiple_of(core * half, 128), half)
    his_cols = pl.ds(pl.multiple_of((1 - core) * half, 128), half)

    def rel(j):
        return lax.rem(chip + j, chips)

    def tok(d, q=None):
        if q is None:
            return pl.ds(pl.multiple_of(d * ctok, ctok), ctok)
        return pl.ds(pl.multiple_of(d * ctok + q * qrows, qrows), qrows)

    def remote(src, dst, slot, target):
        return pltpu.make_async_remote_copy(src_ref=src, dst_ref=dst, send_sem=snd.at[slot], recv_sem=rcv.at[slot],
                                            device_id={'tp': target}, device_id_type=MESH)

    def local(src, dst, i):
        return pltpu.make_async_copy(src, dst, lsem.at[i])

    own_rows = pl.ds(pl.multiple_of(core * qrows, qrows), qrows)
    loads = [local(rp_ref, rp, 0), local(rm_ref, rm, 1), local(keep_ref, keep, 2), local(xchip_ref, xc, 3),
             local(n_ref, n_v, 4), local(dres_ref.at[:, :, my_cols], dres.at[:, own_rows], 5), local(gain_hbm, gain_ref, 6)]
    for cp in loads[:4]:
        cp.start()

    def w_copy(t):
        slot = lax.rem(t, 2)
        return pltpu.make_async_copy(w_ref.at[:, pl.ds(pl.multiple_of(t * u_cols, u_cols), u_cols)], wbuf.at[slot], wsem.at[slot])

    def u_copy(t):
        slot = lax.rem(t, 2)
        return pltpu.make_async_copy(ubuf.at[slot], u_out.at[:, :, pl.ds(pl.multiple_of(t * u_cols, u_cols), u_cols)], usem.at[slot])

    loads[4].start()
    loads[5].start()
    loads[6].start()
    w_copy(0).start()

    barrier = pltpu.get_barrier_semaphore()
    for target in (plus, minus, partner, opposite):
        pl.semaphore_signal(barrier, inc=1, device_id={'tp': target}, device_id_type=MESH)
    pl.semaphore_wait(barrier, 4)

    dres_msg = remote(dres_ref.at[:, :, his_cols], dres.at[:, own_rows], 0, partner)
    dres_msg.start()

    def comb(m, q):
        return remote(s_comb.at[m, q], r_comb.at[m, q], 1 + 2 * m + q, minus if m == 0 else plus)

    def dot_msg(q):
        return remote(dot_s.at[q], dot_r.at[q], 5 + q, partner)

    def spread(q, way):
        here = dxbuf.at[:, tok(chip, q), my_cols]
        return remote(here, here, 7 + 3 * q + way, (plus, minus, partner)[way])

    def far(q, m):
        here = dxbuf.at[m, tok(rel(3 if m == 0 else 1), q), my_cols]
        return remote(here, here, 13 + 2 * q + m, plus if m == 0 else minus)

    def near_fwd(q, side):
        here = dxbuf.at[:, tok(rel(3 if side == 0 else 1), q), my_cols]
        return remote(here, here, 17 + 2 * q + side, partner)

    def far_fwd(q, m):
        here = dxbuf.at[m, tok(rel(2), q), my_cols]
        return remote(here, here, 21 + 2 * q + m, partner)

    def dg_msg(way):
        return remote(dg_v, dg_r.at[way], 25 + way, (plus, minus, opposite)[way])

    dg_fin = remote(dg_half.at[0], dg_half.at[1], 28, partner)

    for cp in loads[:4]:
        cp.wait()
    for q in range(2):
        rows = slice(q * qrows, (q + 1) * qrows)
        s_comb[1, q] = keep[0, rows] + rp[0, rows]
        comb(1, q).start()
        s_comb[0, q] = keep[1, rows] + rm[0, rows]
        comb(0, q).start()
    for cp in loads[4:]:
        cp.wait()
    dres_msg.wait_recv()
    gain_half = gain_ref[my_cols].astype(F32).reshape(1, half)

    def hat_of(m, rows):
        xf = xc[m, rows].astype(F32)
        inv = lax.rsqrt(jnp.mean(xf * xf, axis=-1, keepdims=True) + NORM_EPS)
        return xc[m, rows, my_cols].astype(F32) * inv, inv

    def dn_finish(q):
        rows = slice(q * qrows, (q + 1) * qrows)
        part = jnp.zeros((1, half), F32)
        for m in range(2):
            comb(m, q).wait_recv()
            direct = rp[1, rows] if m == 0 else rm[1, rows]
            dn = keep[2 + m, rows] + direct + r_comb[m, q]
            dn_v[m, rows] = dn
            hat, _ = hat_of(m, rows)
            prod = dn * hat
            part = part + jnp.sum(prod, axis=0, keepdims=True)
            dots = jnp.sum(prod * gain_half, axis=-1, keepdims=True)
            dot_s[q, m] = jnp.broadcast_to(dots, (qrows, 128))
        dot_msg(q).start()
        if q == 0:
            dg_v[...] = part
        else:
            dg_v[...] += part
            for way in range(3):
                dg_msg(way).start()

    def dx_finish(q):
        rows = slice(q * qrows, (q + 1) * qrows)
        dot_msg(q).wait_recv()
        for m in range(2):
            hat, inv = hat_of(m, rows)
            centre = (dot_s[q, m, :, :1] + dot_r[q, m, :, :1]) * (1.0 / model_dim)
            dx = dres[m, rows].astype(F32) + inv * (gain_half * dn_v[m, rows] - hat * centre)
            dxbuf[m, tok(chip, q), my_cols] = dx.astype(BF16)
        for way in range(3):
            spread(q, way).start()

    def near_step(q):
        spread(q, 0).wait_recv()
        far(q, 0).start()
        near_fwd(q, 0).start()
        spread(q, 1).wait_recv()
        far(q, 1).start()
        near_fwd(q, 1).start()

    def far_step(q):
        for m in range(2):
            far(q, m).wait_recv()
            far_fwd(q, m).start()

    def dg_step():
        for way in range(3):
            dg_msg(way).wait_recv()
        dg_half[0] = dg_v[...] + dg_r[0] + dg_r[1] + dg_r[2]
        dg_fin.start()

    hooks = ((U_HOOKS[0], lambda: dn_finish(0)), (U_HOOKS[1], lambda: dx_finish(0)), (U_HOOKS[2], lambda: dn_finish(1)),
             (U_HOOKS[3], lambda: dx_finish(1)), (U_HOOKS[4], lambda: near_step(0)), (U_HOOKS[5], dg_step),
             (U_HOOKS[6], lambda: near_step(1)), (U_HOOKS[7], lambda: far_step(0)))

    def u_step(t, carry):
        @pl.when(t + 1 < steps)
        def _():
            w_copy(t + 1).start()

        w_copy(t).wait()

        @pl.when(t >= 2)
        def _():
            u_copy(t - 2).wait()

        slot = lax.rem(t, 2)
        ubuf[slot] = jnp.dot(n_v[...].reshape(total, model_dim), wbuf[slot], preferred_element_type=F32).astype(BF16).reshape(micro, seq_len, u_cols)
        u_copy(t).start()
        for at, hook in hooks:
            pl.when(t == at)(hook)
        return carry

    lax.fori_loop(0, steps, u_step, 0)
    far_step(1)
    dg_fin.wait_recv()
    dg_copies = [pltpu.make_async_copy(dg_half.at[0], dg_out.at[:, my_cols], osem.at[0]),
                 pltpu.make_async_copy(dg_half.at[1], dg_out.at[:, his_cols], osem.at[1])]
    for cp in dg_copies:
        cp.start()
    for q in range(2):
        spread(q, 2).wait_recv()
        for side in range(2):
            near_fwd(q, side).wait_recv()
    near_copies = [pltpu.make_async_copy(dxbuf.at[:, tok(rel(j))], dx_out.at[:, tok(rel(j))], osem.at[2 + j]) for j in range(chips)]
    for j in (0, 1, 3):
        near_copies[j].start()
    for q in range(2):
        for side in range(2):
            far_fwd(q, side).wait_recv()
    near_copies[2].start()

    for cp in near_copies:
        cp.wait()
    for cp in dg_copies:
        cp.wait()
    u_copy(steps - 2).wait()
    u_copy(steps - 1).wait()
    dres_msg.wait_send()
    dg_fin.wait_send()
    for way in range(3):
        dg_msg(way).wait_send()
    for q in range(2):
        dot_msg(q).wait_send()
        for m in range(2):
            comb(m, q).wait_send()
            far(q, m).wait_send()
            far_fwd(q, m).wait_send()
            near_fwd(q, m).wait_send()
        for way in range(3):
            spread(q, way).wait_send()


def finish_call(group, gain2, rp, rm, keep, xchip, dres, n3, w):
    micro, seq_len, _ = n3.shape
    model_dim, cols_loc = w.shape
    half = model_dim // 2
    chips = group // 2
    ctok = seq_len // chips
    qrows = ctok // 2
    total = micro * seq_len
    hbm_spec = pl.BlockSpec(memory_space=pltpu.HBM)
    any_spec = pl.BlockSpec(memory_space=pl.ANY)
    return pl.pallas_call(
        functools.partial(finish_kernel, group),
        out_shape=(jax.ShapeDtypeStruct((micro, seq_len, cols_loc), BF16),
                   jax.ShapeDtypeStruct((micro, seq_len, model_dim), BF16),
                   jax.ShapeDtypeStruct((1, model_dim), F32)),
        in_specs=[hbm_spec] * 8,
        out_specs=(any_spec,) * 3,
        scratch_shapes=[
            pltpu.VMEM((model_dim,), BF16),
            pltpu.VMEM((2, ctok, half), F32),
            pltpu.VMEM((2, ctok, half), F32),
            pltpu.VMEM((4, ctok, half), F32),
            pltpu.VMEM((micro, ctok, model_dim), BF16),
            pltpu.VMEM((micro, ctok, half), BF16),
            pltpu.VMEM((micro, seq_len, model_dim), BF16),
            pltpu.VMEM((2, model_dim, U_COLS), BF16),
            pltpu.VMEM((2, micro, seq_len, U_COLS), BF16),
            pltpu.VMEM((2, 2, qrows, half), F32),
            pltpu.VMEM((2, 2, qrows, half), F32),
            pltpu.VMEM((micro, ctok, half), F32),
            pltpu.VMEM((2, micro, qrows, 128), F32),
            pltpu.VMEM((2, micro, qrows, 128), F32),
            pltpu.VMEM((micro, seq_len, model_dim), BF16),
            pltpu.VMEM((1, half), F32),
            pltpu.VMEM((3, 1, half), F32),
            pltpu.VMEM((2, 1, half), F32),
            pltpu.SemaphoreType.DMA((7,)),
            pltpu.SemaphoreType.DMA((2,)),
            pltpu.SemaphoreType.DMA((2,)),
            pltpu.SemaphoreType.DMA((2 + chips,)),
            pltpu.SemaphoreType.DMA((29,)),
            pltpu.SemaphoreType.DMA((29,)),
        ],
        compiler_params=pltpu.CompilerParams(collective_id=1, has_side_effects=True, vmem_limit_bytes=30 * 1024 * 1024),
        cost_estimate=pl.CostEstimate(flops=2 * total * cols_loc * model_dim, bytes_accessed=2 * cols_loc * model_dim, transcendentals=0),
        name="finish_u",
    )(*[pltpu.with_memory_space_constraint(v, pltpu.HBM) for v in (gain2, rp, rm, keep, xchip, dres, n3, w)])


def epilogue_kernel(ids_ref, u_ref, dx_ref, dg_ref, xchip_ref, u_out, de_out, dg_out, x_out, u_v, dx_v, de_v, x_v, usem, xsem, osem):
    dev = lax.axis_index('tp')
    own_tok = x_v.shape[1]
    own_rows = pl.ds(pl.multiple_of(lax.rem(dev, 2) * own_tok, own_tok), own_tok)
    own_in = pltpu.make_async_copy(xchip_ref.at[:, own_rows], x_v, osem.at[0])
    own_out = pltpu.make_async_copy(x_v, x_out, osem.at[1])
    micro, seq_len = ids_ref.shape
    rows_loc, model_dim = de_v.shape
    steps = model_dim // DE_COLS
    ucols = u_v.shape[2] // U_PARTS

    def cols(i, n):
        return pl.ds(i * n, n)

    x_loads = [pltpu.make_async_copy(dx_ref.at[:, :, cols(i, DE_COLS)], dx_v.at[:, :, cols(i, DE_COLS)], xsem.at[i]) for i in range(steps)]
    u_loads = [pltpu.make_async_copy(u_ref.at[:, :, cols(i, ucols)], u_v.at[:, :, cols(i, ucols)], usem.at[i]) for i in range(U_PARTS)]
    x_loads[0].start()
    x_loads[1].start()
    for cp in u_loads:
        cp.start()
    for cp in x_loads[2:]:
        cp.start()
    own_in.start()
    dg_out[...] = dg_ref[0]
    row_id = lax.broadcasted_iota(jnp.int32, (rows_loc, seq_len), 0) + dev * rows_loc
    hot = jnp.concatenate([jnp.where(row_id == ids_ref[m:m + 1, :], 1.0, 0.0).astype(BF16) for m in range(micro)], axis=1)
    u_stores = [pltpu.make_async_copy(u_v.at[:, :, cols(i, ucols)], u_out.at[:, :, cols(i, ucols)], usem.at[U_PARTS + i]) for i in range(U_PARTS)]
    de_stores = [pltpu.make_async_copy(de_v.at[:, cols(i, DE_COLS)], de_out.at[:, cols(i, DE_COLS)], xsem.at[steps + i]) for i in range(steps)]
    for i in range(steps):
        x_loads[i].wait()
        de_v[:, cols(i, DE_COLS)] = jnp.dot(hot, dx_v[:, :, cols(i, DE_COLS)].reshape(micro * seq_len, DE_COLS), preferred_element_type=F32)
        de_stores[i].start()
        if i < U_PARTS:
            u_loads[i].wait()
            u_stores[i].start()
    own_in.wait()
    own_out.start()
    for cp in u_stores + de_stores + [own_out]:
        cp.wait()


def epilogue_call(rows_loc, ids, u, dx, dg, xchip):
    micro, seq_len, _ = u.shape
    model_dim = dx.shape[2]
    steps = model_dim // DE_COLS
    any_spec = pl.BlockSpec(memory_space=pl.ANY)
    vmem_spec = pl.BlockSpec(memory_space=pltpu.VMEM)
    return pl.pallas_call(
        epilogue_kernel,
        out_shape=(jax.ShapeDtypeStruct(u.shape, BF16), jax.ShapeDtypeStruct((rows_loc, model_dim), F32),
                   jax.ShapeDtypeStruct((model_dim,), F32),
                   jax.ShapeDtypeStruct((micro, xchip.shape[1] // 2, model_dim), BF16)),
        in_specs=[vmem_spec, any_spec, any_spec, vmem_spec, any_spec],
        out_specs=(any_spec, any_spec, vmem_spec, any_spec),
        scratch_shapes=[
            pltpu.VMEM(u.shape, BF16),
            pltpu.VMEM(dx.shape, BF16),
            pltpu.VMEM((rows_loc, model_dim), F32),
            pltpu.VMEM((micro, xchip.shape[1] // 2, model_dim), BF16),
            pltpu.SemaphoreType.DMA((2 * U_PARTS,)),
            pltpu.SemaphoreType.DMA((2 * steps,)),
            pltpu.SemaphoreType.DMA((2,)),
        ],
        compiler_params=pltpu.CompilerParams(vmem_limit_bytes=22 * 1024 * 1024),
        cost_estimate=pl.CostEstimate(flops=2 * micro * seq_len * rows_loc * model_dim, bytes_accessed=4 * rows_loc * model_dim, transcendentals=0),
        name="epilogue",
    )(ids, u, dx, dg, xchip)


def solution(mesh):
    group = mesh.shape['tp']
    plus = [(r, (r + 2) % group) for r in range(group)]
    minus = [(r, (r - 2) % group) for r in range(group)]

    def local_step(token_ids, table_loc, gain_vec, w_loc, du_loc, dres_loc):
        micro, seq_len = token_ids.shape
        model_dim, cols_loc = w_loc.shape
        total = micro * seq_len
        gain2 = gain_vec
        normed, x_chip, msg_plus, msg_minus, keep = gather_call(group, token_ids, gain2, table_loc, w_loc, du_loc)
        got_plus = lax.ppermute(msg_plus, 'tp', plus)
        got_minus = lax.ppermute(msg_minus, 'tp', minus)
        grad_w = weight_grad_call(normed.reshape(total, model_dim), du_loc.reshape(total, cols_loc))
        u_tmp, dx_all, dg = finish_call(group, gain2, got_plus, got_minus, keep, x_chip, dres_loc, normed, w_loc)
        u, grad_table, grad_gain, x_own = epilogue_call(table_loc.shape[0], token_ids, u_tmp, dx_all, dg, x_chip)
        return u, x_own, grad_table, grad_w, grad_gain

    return jax.shard_map(local_step, mesh=mesh,
                         in_specs=(P('dp', None), P('tp', None), P(None), P(None, 'tp'), P('dp', None, 'tp'), P('dp', 'tp', None)),
                         out_specs=(P('dp', None, 'tp'), P('dp', 'tp', None), P(('dp', 'tp'), None), P(None, ('dp', 'tp')), P('dp')),
                         check_vma=False)
```
